8 devices in a mesh: dp: 1 (over z), tp: 8 (over y, x, core).
Axes of the slice: x: 2, y: 2, z: 1, core: 2. Of those that a mesh axis runs over, the one named last changes fastest.
Arguments:
- hidden: bfloat16 [4, 4096, 2048], P('dp', 'tp')
- attn_gain: float32 [2048], replicated
- w_q: bfloat16 [2048, 2048], P(None, 'tp')
- w_k: bfloat16 [2048, 2048], P(None, 'tp')
- w_v: bfloat16 [2048, 2048], P(None, 'tp')
- q_gain: float32 [2048], P('tp')
- k_gain: float32 [2048], P('tp')
- w_o: bfloat16 [2048, 2048], P('tp')
Outputs:
- output 1: bfloat16 [4, 4096, 2048], P('dp', 'tp')
- output 2: bfloat16 [4, 4096, 16, 128], P('dp', None, 'tp')
- output 3: bfloat16 [4, 4096, 16, 128], P('dp', None, 'tp')
All inputs are finite; a program needn't handle non-finite values.
Results may differ from the reference program's by a relative error of at most 0.009045.
Values are sent between devices in bfloat16 or wider.
A program may use at most 1 GiB of HBM per device.

```python
import jax
import jax.numpy as jnp
from jax import lax

BATCH_SIZE = 4
SEQ_LEN = 4096
D_MODEL = 2048
N_HEADS = 16
HEAD_DIM = 128


def setup_inputs(seed: int = 0, part: int = 0) -> dict:
    base_key = jax.random.key(seed)
    part_keys = jax.random.split(jax.random.fold_in(base_key, part), 2)
    key_list = jax.random.split(base_key, 9)
    x_noise = jax.random.normal(part_keys[0], (BATCH_SIZE, SEQ_LEN, D_MODEL), jnp.float32)
    x_mean = jax.random.normal(part_keys[1], (BATCH_SIZE, 1, D_MODEL), jnp.float32)
    head_pos = jnp.arange(N_HEADS, dtype=jnp.float32) / max(N_HEADS - 1, 1)
    q_heads = 10.0 ** (head_pos - 0.5) * jax.random.uniform(key_list[0], (N_HEADS,), jnp.float32, 0.8, 1.2)
    k_heads = 10.0 ** (0.5 - head_pos) * jax.random.uniform(key_list[1], (N_HEADS,), jnp.float32, 0.8, 1.2)
    fan_scale = D_MODEL ** -0.5
    w_shape = (D_MODEL, D_MODEL)
    w_q = jax.random.normal(key_list[2], w_shape, jnp.float32) * (fan_scale * jnp.repeat(q_heads, HEAD_DIM))[None, :]
    w_k = jax.random.normal(key_list[3], w_shape, jnp.float32) * (fan_scale * jnp.repeat(k_heads, HEAD_DIM))[None, :]
    w_v = jax.random.normal(key_list[4], w_shape, jnp.float32) * fan_scale
    w_o = jax.random.normal(key_list[5], w_shape, jnp.float32) * fan_scale
    return {
        'hidden': (x_noise + x_mean).astype(jnp.bfloat16),
        'attn_gain': jax.random.uniform(key_list[6], (D_MODEL,), jnp.float32, 0.5, 1.5),
        'w_q': w_q.astype(jnp.bfloat16),
        'w_k': w_k.astype(jnp.bfloat16),
        'w_v': w_v.astype(jnp.bfloat16),
        'q_gain': jax.random.uniform(key_list[7], (D_MODEL,), jnp.float32, 1.5, 3.5),
        'k_gain': jax.random.uniform(key_list[8], (D_MODEL,), jnp.float32, 1.5, 3.5),
        'w_o': w_o.astype(jnp.bfloat16),
    }


def rope_tables(seq_len, head_dim):
    half_dim = head_dim // 2
    inv_freq = 10000.0 ** (-jnp.arange(half_dim, dtype=jnp.float32) * (2.0 / head_dim))
    angles = jnp.arange(seq_len, dtype=jnp.float32)[:, None] * inv_freq[None, :]
    return jnp.cos(angles), jnp.sin(angles)


def apply_rope(heads_in, cos_tab, sin_tab):
    half_dim = heads_in.shape[-1] // 2
    lower_half = heads_in[..., :half_dim]
    upper_half = heads_in[..., half_dim:]
    cos_bcast = cos_tab[None, :, None, :]
    sin_bcast = sin_tab[None, :, None, :]
    return jnp.concatenate([lower_half * cos_bcast - upper_half * sin_bcast, upper_half * cos_bcast + lower_half * sin_bcast], axis=-1)


def reference(hidden, attn_gain, w_q, w_k, w_v, q_gain, k_gain, w_o):
    x_f32 = hidden.astype(jnp.float32)
    inv_rms = lax.rsqrt(jnp.mean(x_f32 * x_f32, axis=-1, keepdims=True) + 1e-5)
    h_rows = (x_f32 * inv_rms * attn_gain).astype(jnp.bfloat16).reshape(BATCH_SIZE * SEQ_LEN, D_MODEL)
    q_raw = jnp.dot(h_rows, w_q, preferred_element_type=jnp.float32).astype(jnp.bfloat16).astype(jnp.float32)
    k_raw = jnp.dot(h_rows, w_k, preferred_element_type=jnp.float32).astype(jnp.bfloat16).astype(jnp.float32)
    v_rows = jnp.dot(h_rows, w_v, preferred_element_type=jnp.float32).astype(jnp.bfloat16)
    q_normed = q_raw * lax.rsqrt(jnp.mean(q_raw * q_raw, axis=-1, keepdims=True) + 1e-5) * q_gain
    k_normed = k_raw * lax.rsqrt(jnp.mean(k_raw * k_raw, axis=-1, keepdims=True) + 1e-5) * k_gain
    cos_tab, sin_tab = rope_tables(SEQ_LEN, HEAD_DIM)
    head_shape = (BATCH_SIZE, SEQ_LEN, N_HEADS, HEAD_DIM)
    q_rot = apply_rope(q_normed.reshape(head_shape), cos_tab, sin_tab).astype(jnp.bfloat16)
    k_rot = apply_rope(k_normed.reshape(head_shape), cos_tab, sin_tab).astype(jnp.bfloat16)
    v_heads = v_rows.reshape(head_shape)
    positions = jnp.arange(SEQ_LEN)
    causal = positions[:, None] >= positions[None, :]
    score_scale = HEAD_DIM ** -0.5

    def one_head(head_args):
        q_head, k_head, v_head = head_args
        scores = jnp.einsum('bqd,bkd->bqk', q_head.astype(jnp.float32), k_head.astype(jnp.float32)) * score_scale
        scores = jnp.where(causal[None], scores, -1e30)
        prob_bf = jax.nn.softmax(scores, axis=-1).astype(jnp.bfloat16)
        head_out = jnp.einsum('bqk,bkd->bqd', prob_bf.astype(jnp.float32), v_head.astype(jnp.float32))
        return head_out.astype(jnp.bfloat16)

    per_head = lax.map(one_head, (jnp.moveaxis(q_rot, 2, 0), jnp.moveaxis(k_rot, 2, 0), jnp.moveaxis(v_heads, 2, 0)))
    attn_rows = jnp.moveaxis(per_head, 0, 2).reshape(BATCH_SIZE * SEQ_LEN, D_MODEL)
    y_rows = jnp.dot(attn_rows, w_o, preferred_element_type=jnp.float32).astype(jnp.bfloat16)
    hidden_out = (x_f32 + y_rows.reshape(hidden.shape).astype(jnp.float32)).astype(jnp.bfloat16)
    return (hidden_out, k_rot, v_heads)
```

```python
import functools
import math

import jax
import jax.numpy as jnp
from jax import lax
from jax.experimental import pallas as pl
from jax.experimental.pallas import tpu as pltpu
from jax.sharding import PartitionSpec as P

HEAD_DIM = 128
EPS = 1e-5
MESH = pl.DeviceIdType.MESH


def rope_tables(seq_len):
    half_dim = HEAD_DIM // 2
    inv_freq = 10000.0 ** (-jnp.arange(half_dim, dtype=jnp.float32) * (2.0 / HEAD_DIM))
    angles = jnp.arange(seq_len, dtype=jnp.float32)[:, None] * inv_freq[None, :]
    cos, sin = jnp.cos(angles), jnp.sin(angles)
    return jnp.concatenate([cos, cos], axis=1), jnp.concatenate([-sin, sin], axis=1)


def block_kernel(n, width, h_ref, wq_ref, wk_ref, wv_ref, qg_ref, kg_ref, cos_ref, sin_ref,
                 o_hbm, k_out, v_out,
                 q_s, k_s, vt_s, stats, o_s, st_send, st_recv, o_send, o_recv, o_local):
    step = pl.program_id(0)
    me = lax.axis_index('tp')
    tile = h_ref.shape[0]
    cols = wq_ref.shape[1]
    heads = cols // HEAD_DIM
    groups = tile // HEAD_DIM
    half = n // 2

    def peer(d):
        return {'tp': lax.rem(me + d, n)}

    def stats_copy(chunk, d):
        part = stats.at[me, pl.ds(chunk * half, half)]
        return pltpu.make_async_remote_copy(
            src_ref=part, dst_ref=part, send_sem=st_send.at[d, chunk], recv_sem=st_recv.at[me, chunk],
            device_id=peer(d), device_id_type=MESH)

    def wait_stats(chunk):
        for d in range(1, n):
            src = lax.rem(me + d, n)
            part = stats.at[src, pl.ds(chunk * half, half)]
            pltpu.make_async_remote_copy(
                src_ref=part, dst_ref=part, send_sem=st_send.at[d, chunk], recv_sem=st_recv.at[src, chunk],
                device_id=peer(d), device_id_type=MESH).wait_recv()

    @pl.when(step == 0)
    def _():
        barrier = pltpu.get_barrier_semaphore()
        for d in range(1, n):
            pl.semaphore_signal(barrier, inc=1, device_id=peer(d), device_id_type=MESH)

    @pl.when(step == half)
    def _():
        pl.semaphore_wait(pltpu.get_barrier_semaphore(), n - 1)
        for d in range(1, n):
            stats_copy(0, d).start()

    @pl.when(step < n)
    def _():
        h = h_ref[...]
        q = jnp.dot(h, wq_ref[...], preferred_element_type=jnp.float32).astype(jnp.bfloat16)
        k = jnp.dot(h, wk_ref[...], preferred_element_type=jnp.float32).astype(jnp.bfloat16)
        v = jnp.dot(h, wv_ref[...], preferred_element_type=jnp.float32).astype(jnp.bfloat16)
        q_s[step] = q
        k_s[step] = k
        v_out[...] = v
        vt_s[step] = v.T
        qf, kf = q.astype(jnp.float32), k.astype(jnp.float32)
        q_sq = jnp.sum(qf * qf, axis=1, keepdims=True)
        k_sq = jnp.sum(kf * kf, axis=1, keepdims=True)
        lane = lax.broadcasted_iota(jnp.int32, (HEAD_DIM, HEAD_DIM), 1)
        rows = []
        for g in range(groups):
            part = slice(g * HEAD_DIM, (g + 1) * HEAD_DIM)
            both = jnp.where(lane == 0, q_sq[part], k_sq[part])
            rows.append(both.T[:2])
        stats[me, step] = jnp.concatenate(rows, axis=0)

    @pl.when(step == n)
    def _():
        for d in range(1, n):
            stats_copy(1, d).start()
        wait_stats(0)

    @pl.when(step == n + half)
    def _():
        wait_stats(1)

    @pl.when((step >= n) & (step < 2 * n))
    def _():
        j = step - n
        total = stats[0, j]
        for s in range(1, n):
            total = total + stats[s, j]
        inv = lax.rsqrt(total / width + EPS)
        inv_cols = jnp.concatenate([inv] * (HEAD_DIM // inv.shape[0]), axis=0).T
        for g in range(groups):
            part = slice(g * HEAD_DIM, (g + 1) * HEAD_DIM)
            cos, sin = cos_ref[part, :], sin_ref[part, :]
            for x_s, g_ref, col in ((q_s, qg_ref, 2 * g), (k_s, kg_ref, 2 * g + 1)):
                x = x_s[j, part, :].astype(jnp.float32) * inv_cols[:, col:col + 1] * g_ref[...]
                outs = []
                for hd in range(heads):
                    xh = x[:, hd * HEAD_DIM:(hd + 1) * HEAD_DIM]
                    outs.append((xh * cos + pltpu.roll(xh, HEAD_DIM // 2, 1) * sin).astype(jnp.bfloat16))
                rot = jnp.concatenate(outs, axis=1)
                x_s[j, part, :] = rot
                if x_s is k_s:
                    k_out[part, :] = rot

    def o_copy(d):
        return pltpu.make_async_remote_copy(
            src_ref=o_s.at[d], dst_ref=o_hbm.at[:, pl.ds(pl.multiple_of(me * cols, cols), cols)],
            send_sem=o_send.at[d], recv_sem=o_recv.at[me], device_id=peer(d), device_id_type=MESH)

    def o_own():
        return pltpu.make_async_copy(o_s.at[0], o_hbm.at[:, pl.ds(pl.multiple_of(me * cols, cols), cols)], o_local)

    @pl.when(step >= 2 * n)
    def _():
        d = lax.rem(step - 2 * n + 1, n)
        blk = lax.rem(me + d, n)
        scale = HEAD_DIM ** -0.5 * math.log2(math.e)
        nt = (((1,), (1,)), ((), ()))

        def hcols(hd):
            return slice(hd * HEAD_DIM, (hd + 1) * HEAD_DIM)

        qs = [q_s[blk, :, hcols(hd)] for hd in range(heads)]

        def scores(j, hd):
            return lax.dot_general(k_s[j, :, hcols(hd)], qs[hd], nt, preferred_element_type=jnp.float32)

        key_pos = lax.broadcasted_iota(jnp.int32, (tile, tile), 0)
        query_pos = lax.broadcasted_iota(jnp.int32, (tile, tile), 1)
        keep = key_pos <= query_pos
        carry = []
        for hd in range(heads):
            s = jnp.where(keep, scores(blk, hd), -jnp.inf)
            m = jnp.max(s, axis=0, keepdims=True)
            p = jnp.exp2(s * scale - m * scale)
            l = jnp.sum(p, axis=0, keepdims=True)
            acc = jnp.dot(vt_s[blk, hcols(hd), :], p.astype(jnp.bfloat16), preferred_element_type=jnp.float32)
            carry.append((m, l, acc))

        def body(j, carry):
            out = []
            ss = [scores(j, hd) for hd in range(heads)]
            for hd in range(heads):
                m, l, acc = carry[hd]
                s = ss[hd]
                m_new = jnp.maximum(m, jnp.max(s, axis=0, keepdims=True))
                alpha = jnp.exp2((m - m_new) * scale)
                p = jnp.exp2(s * scale - m_new * scale)
                l = l * alpha + jnp.sum(p, axis=0, keepdims=True)
                acc = acc * alpha + jnp.dot(vt_s[j, hcols(hd), :], p.astype(jnp.bfloat16), preferred_element_type=jnp.float32)
                out.append((m_new, l, acc))
            return tuple(out)

        carry = lax.fori_loop(0, blk, body, tuple(carry))
        for hd in range(heads):
            m, l, acc = carry[hd]
            o_s[d, :, hcols(hd)] = (acc / l).T.astype(jnp.bfloat16)

        @pl.when(d != 0)
        def _():
            o_copy(d).start()

        @pl.when(d == 0)
        def _():
            o_own().start()

    @pl.when(step == 3 * n - 1)
    def _():
        o_own().wait()
        for d in range(1, n):
            src = lax.rem(me + d, n)
            o_copy(d).wait_send()
            pltpu.make_async_remote_copy(
                src_ref=o_s.at[d], dst_ref=o_hbm.at[:, pl.ds(pl.multiple_of(src * cols, cols), cols)],
                send_sem=o_send.at[d], recv_sem=o_recv.at[src], device_id=peer(d), device_id_type=MESH).wait_recv()
            for chunk in range(2):
                stats_copy(chunk, d).wait_send()


def block_call(n, h_full, wq, wk, wv, qg, kg, cos, sin):
    seq, width = h_full.shape
    cols = wq.shape[1]
    tile = seq // n
    heads = cols // HEAD_DIM

    def first(i):
        return (jnp.minimum(i, n - 1), 0)

    def second(i):
        return (jnp.clip(i - n, 0, n - 1), 0)

    def whole(i):
        return (0, 0)

    flops = 2 * seq * width * cols * 3 + 2 * seq * seq * cols * 2
    return pl.pallas_call(
        functools.partial(block_kernel, n, width),
        grid=(3 * n,),
        in_specs=[
            pl.BlockSpec((tile, width), first),
            pl.BlockSpec((width, cols), whole), pl.BlockSpec((width, cols), whole), pl.BlockSpec((width, cols), whole),
            pl.BlockSpec((1, cols), whole), pl.BlockSpec((1, cols), whole),
            pl.BlockSpec((tile, HEAD_DIM), second), pl.BlockSpec((tile, HEAD_DIM), second),
        ],
        out_specs=[
            pl.BlockSpec(memory_space=pl.ANY),
            pl.BlockSpec((tile, cols), second),
            pl.BlockSpec((tile, cols), first),
        ],
        out_shape=[
            jax.ShapeDtypeStruct((tile, n * cols), jnp.bfloat16),
            jax.ShapeDtypeStruct((seq, cols), jnp.bfloat16),
            jax.ShapeDtypeStruct((seq, cols), jnp.bfloat16),
        ],
        scratch_shapes=[
            pltpu.VMEM((n, tile, cols), jnp.bfloat16),
            pltpu.VMEM((n, tile, cols), jnp.bfloat16),
            pltpu.VMEM((n, cols, tile), jnp.bfloat16),
            pltpu.VMEM((n, n, 2 * tile // HEAD_DIM, HEAD_DIM), jnp.float32),
            pltpu.VMEM((n, tile, cols), jnp.bfloat16),
            pltpu.SemaphoreType.DMA((n, 2)),
            pltpu.SemaphoreType.DMA((n, 2)),
            pltpu.SemaphoreType.DMA((n,)),
            pltpu.SemaphoreType.DMA((n,)),
            pltpu.SemaphoreType.DMA,
        ],
        compiler_params=pltpu.CompilerParams(
            collective_id=0, has_side_effects=True, vmem_limit_bytes=52 * 1024 * 1024,
            dimension_semantics=('arbitrary',)),
        cost_estimate=pl.CostEstimate(flops=flops, bytes_accessed=seq * width * 2 + 6 * seq * cols * 2, transcendentals=seq * seq * heads // 2),
        name='attn_block',
    )(h_full, wq, wk, wv, qg, kg, cos, sin)


def solution(mesh):
    n = mesh.shape['tp']

    def local_block(x_local, attn_gain, wq, wk, wv, qg, kg, wo_rows):
        n_batch, rows, width = x_local.shape
        seq = rows * n
        cols = wq.shape[1]
        cos, sin = rope_tables(seq)
        qg2, kg2 = qg.reshape(1, cols), kg.reshape(1, cols)
        gathered = []
        for b in range(n_batch):
            x_f32 = x_local[b].astype(jnp.float32)
            inv_rms = lax.rsqrt(jnp.mean(x_f32 * x_f32, axis=-1, keepdims=True) + EPS)
            normed = (x_f32 * inv_rms * attn_gain).astype(jnp.bfloat16)
            gathered.append(lax.all_gather(normed, 'tp', axis=0, tiled=True))
        wo_src, gathered[-1] = lax.optimization_barrier((wo_rows, gathered[-1]))
        w_o = lax.all_gather(wo_src, 'tp', axis=0, tiled=True)
        os, ks, vs = [], [], []
        for b in range(n_batch):
            o, k, v = block_call(n, gathered[b], wq, wk, wv, qg2, kg2, cos, sin)
            os.append(o)
            ks.append(k)
            vs.append(v)
        o_all = jnp.stack(os)
        y = jnp.einsum('btc,cd->btd', o_all, w_o, preferred_element_type=jnp.float32).astype(jnp.bfloat16)
        hidden_out = (x_local.astype(jnp.float32) + y.astype(jnp.float32)).astype(jnp.bfloat16)
        cache_shape = (n_batch, seq, cols // HEAD_DIM, HEAD_DIM)
        return hidden_out, jnp.stack(ks).reshape(cache_shape), jnp.stack(vs).reshape(cache_shape)

    seq_spec = P('dp', 'tp', None)
    head_spec = P('dp', None, 'tp', None)
    col_spec = P(None, 'tp')
    return jax.shard_map(local_block, mesh=mesh, in_specs=(seq_spec, P(None), col_spec, col_spec, col_spec, P('tp'), P('tp'), P('tp', None)), out_specs=(seq_spec, head_spec, head_spec), check_vma=False)
```

```python
import functools
import math

import jax
import jax.numpy as jnp
from jax import lax
from jax.experimental import pallas as pl
from jax.experimental.pallas import tpu as pltpu
from jax.sharding import PartitionSpec as P

HEAD_DIM = 128
EPS = 1e-5
MESH = pl.DeviceIdType.MESH


FIRST = ((0, 2), (2, 1), (3, 1), (4, 4))
SECOND = ((4, 2), (6, 1), (7, 1), (0, 4))
PIECES = FIRST + SECOND + ((4, 4), (0, 4))
LAST = len(PIECES)


class RingGather:
    def __init__(self, buf, own, stage, me, ici_send, ici_recv, d2d_send, d2d_recv, keep):
        self.buf, self.own, self.stage, self.me, self.rows = buf, own, stage, me, own.shape[0]
        self.ici_send, self.ici_recv, self.d2d_send, self.d2d_recv, self.keep = ici_send, ici_recv, d2d_send, d2d_recv, keep
        self.xn = me + 2 - 4 * lax.rem(me // 2, 2)
        self.yn = me + 4 - 8 * (me // 4)
        self.dg = self.yn + 2 - 4 * lax.rem(me // 2, 2)
        self.pt = me + 1 - 2 * lax.rem(me, 2)

    def block(self, block):
        return self.buf.at[pl.ds(pl.multiple_of(block * self.rows, self.rows), self.rows)]

    def span(self, piece):
        unit = self.rows // 8
        return PIECES[piece][0] * unit, PIECES[piece][1] * unit

    def slot(self, block, piece):
        first, rows = self.span(piece)
        unit = self.rows // 8
        return self.buf.at[pl.ds(pl.multiple_of(block * self.rows + first, unit), rows)]

    def staged(self, piece):
        first, rows = self.span(piece)
        which = 0 if piece < 4 else 1 if piece < 8 else 2
        return self.stage.at[which, pl.ds(first, rows)]

    def source(self, piece):
        return self.xn if piece < 4 else self.yn if piece < 8 else self.dg

    def copy(self, piece):
        first, rows = self.span(piece)
        if piece < 8:
            src = self.own.at[pl.ds(first, rows)]
        else:
            src = self.stage.at[1 if piece == 8 else 0, pl.ds(first, rows)]
        return pltpu.make_async_remote_copy(
            src_ref=src, dst_ref=self.staged(piece), send_sem=self.ici_send.at[piece], recv_sem=self.ici_recv.at[piece],
            device_id={'tp': self.xn if piece < 4 or piece == 8 else self.yn}, device_id_type=MESH)

    def handover(self, piece):
        if piece == LAST:
            src, dst = self.own, self.block(self.me)
        else:
            src, dst = self.staged(piece), self.slot(self.source(piece), piece)
        return pltpu.make_async_remote_copy(
            src_ref=src, dst_ref=dst, send_sem=self.d2d_send.at[piece], recv_sem=self.d2d_recv.at[piece],
            device_id={'tp': self.pt}, device_id_type=MESH)

    def store(self, piece):
        return pltpu.make_async_copy(self.staged(piece), self.slot(self.source(piece), piece), self.keep.at[piece])

    def send(self, turns):
        for turn in turns:
            self.copy(turn).start()
            self.copy(4 + turn).start()
        if 3 in turns:
            self.handover(LAST).start()

    def relay(self):
        for turns, onward in (((0, 1, 2), 9), ((4, 5, 6), 8)):
            for piece in turns:
                self.copy(piece).wait_recv()
            self.copy(onward).start()
        self.pass_on((0, 1, 2, 4, 5, 6))

    def pass_on(self, pieces):
        for piece in pieces:
            self.handover(piece).start()
            self.store(piece).start()

    def take(self, pieces):
        for piece in pieces:
            self.copy(piece).wait_recv()
            self.pass_on((piece,))

    def finish(self):
        self.take((8, 9))
        for piece in range(LAST):
            self.copy(piece).wait_send()
            self.store(piece).wait()
        for piece in range(LAST + 1):
            src = self.pt if piece == LAST else self.pt + self.source(piece) - self.me
            part = self.block(src) if piece == LAST else self.slot(src, piece)
            pltpu.make_async_remote_copy(
                src_ref=part, dst_ref=part, send_sem=self.d2d_send.at[piece], recv_sem=self.d2d_recv.at[piece],
                device_id={'tp': self.pt}, device_id_type=MESH).wait_recv()
            self.handover(piece).wait_send()


GATHER_SEMS = [pltpu.SemaphoreType.DMA((LAST,)), pltpu.SemaphoreType.DMA((LAST,)),
               pltpu.SemaphoreType.DMA((LAST + 1,)), pltpu.SemaphoreType.DMA((LAST + 1,)), pltpu.SemaphoreType.DMA((LAST,))]


def greet(n, me):
    barrier = pltpu.get_barrier_semaphore()
    for d in range(1, n):
        pl.semaphore_signal(barrier, inc=1, device_id={'tp': lax.rem(me + d, n)}, device_id_type=MESH)


def first_kernel(n, n_batch, x_hbm, gain_ref, wo_hbm, freq_ref,
                 h0, h1, h2, h3, wo_full, cos_hbm, sin_hbm,
                 x_v, h_v, wo_v, stage, cos_v, sin_v, in_sem, wo_sem, out_sem, tab_sem, *gather_sems):
    me = lax.axis_index('tp')
    rows, width = x_v.shape[1:]
    wo_rows = wo_v.shape[0]
    hs = (h0, h1, h2, h3)
    greet(n, me)
    loads = [pltpu.make_async_copy(x_hbm.at[b], x_v.at[b], in_sem.at[b]) for b in range(n_batch)]
    wo_load = pltpu.make_async_copy(wo_hbm, wo_v, wo_sem.at[0])
    wo_store = pltpu.make_async_copy(wo_v, wo_full.at[pl.ds(pl.multiple_of(me * wo_rows, wo_rows), wo_rows)], wo_sem.at[1])
    stores = [pltpu.make_async_copy(h_v.at[b], hs[b].at[pl.ds(pl.multiple_of(me * rows, rows), rows)], out_sem.at[b])
              for b in range(n_batch)]
    loads[0].start()

    def norm(b):
        def body(r, carry):
            part = pl.ds(pl.multiple_of(r * 64, 64), 64)
            x = x_v[b, part, :].astype(jnp.float32)
            inv = lax.rsqrt(jnp.mean(x * x, axis=-1, keepdims=True) + EPS)
            h_v[b, part, :] = (x * inv * gain_ref[...]).astype(jnp.bfloat16)
            return carry
        lax.fori_loop(0, rows // 64, body, 0)

    loads[0].wait()
    for load in loads[1:]:
        load.start()
    wo_load.start()
    norm(0)
    pl.semaphore_wait(pltpu.get_barrier_semaphore(), n - 1)
    gather = RingGather(h0, h_v.at[0], stage, me, *gather_sems)
    gather.send((0, 1, 2, 3))
    stores[0].start()
    for b in range(1, n_batch):
        loads[b].wait()
        norm(b)
        stores[b].start()
    wo_load.wait()
    wo_store.start()
    seq = cos_v.shape[0]

    def table(r, carry):
        part = pl.ds(pl.multiple_of(r * 64, 64), 64)
        pos = (lax.broadcasted_iota(jnp.int32, (64, HEAD_DIM), 0) + r * 64).astype(jnp.float32)
        lane = lax.broadcasted_iota(jnp.int32, (64, HEAD_DIM), 1)
        angle = pos * freq_ref[...]
        sin = jnp.sin(angle)
        cos_v[part, :] = jnp.cos(angle)
        sin_v[part, :] = jnp.where(lane < HEAD_DIM // 2, -sin, sin)
        return carry

    lax.fori_loop(0, seq // 64, table, 0)
    tables = [pltpu.make_async_copy(cos_v, cos_hbm, tab_sem.at[0]), pltpu.make_async_copy(sin_v, sin_hbm, tab_sem.at[1])]
    for copy in tables:
        copy.start()
    gather.relay()
    gather.take((3, 7))
    for copy in stores + [wo_store] + tables:
        copy.wait()
    gather.finish()


def first_call(n, x_local, gain, wo_rows, freq):
    n_batch, rows, width = x_local.shape
    depth = wo_rows.shape[0]
    seq = n * rows
    hbm = pl.BlockSpec(memory_space=pl.ANY)
    vmem = pl.BlockSpec(memory_space=pltpu.VMEM)
    return pl.pallas_call(
        functools.partial(first_kernel, n, n_batch),
        in_specs=[hbm, vmem, hbm, vmem],
        out_specs=[hbm] * (n_batch + 3),
        out_shape=[jax.ShapeDtypeStruct((seq, width), jnp.bfloat16)] * n_batch
        + [jax.ShapeDtypeStruct((n * depth, width), jnp.bfloat16)]
        + [jax.ShapeDtypeStruct((seq, HEAD_DIM), jnp.float32)] * 2,
        scratch_shapes=[
            pltpu.VMEM((n_batch, rows, width), jnp.bfloat16),
            pltpu.VMEM((n_batch, rows, width), jnp.bfloat16),
            pltpu.VMEM((depth, width), jnp.bfloat16),
            pltpu.VMEM((3, rows, width), jnp.bfloat16),
            pltpu.VMEM((seq, HEAD_DIM), jnp.float32),
            pltpu.VMEM((seq, HEAD_DIM), jnp.float32),
            pltpu.SemaphoreType.DMA((n_batch,)),
            pltpu.SemaphoreType.DMA((2,)),
            pltpu.SemaphoreType.DMA((n_batch,)),
            pltpu.SemaphoreType.DMA((2,)),
        ] + GATHER_SEMS,
        compiler_params=pltpu.CompilerParams(
            collective_id=0, has_side_effects=True, vmem_limit_bytes=40 * 1024 * 1024),
        cost_estimate=pl.CostEstimate(flops=100000000, bytes_accessed=seq * width * 4, transcendentals=seq * HEAD_DIM * 2),
        name='first_gather',
    )(x_local, gain, wo_rows, freq)


def block_kernel(n, width, h_ref, wq_ref, wk_ref, wv_ref, qg_ref, kg_ref, cos_ref, sin_ref, next_in,
                 o_hbm, next_buf, k_out, v_out,
                 q_s, k_s, vt_s, stats, o_s, own_v, stage, own_sem, st_send, st_recv, o_send, o_recv, o_local, *gather_sems):
    step = pl.program_id(0)
    me = lax.axis_index('tp')
    tile = h_ref.shape[0]
    cols = wq_ref.shape[1]
    heads = cols // HEAD_DIM
    groups = tile // HEAD_DIM
    half = n // 2

    def peer(d):
        return {'tp': lax.rem(me + d, n)}

    def stats_copy(chunk, d):
        part = stats.at[me, pl.ds(chunk * half, half)]
        return pltpu.make_async_remote_copy(
            src_ref=part, dst_ref=part, send_sem=st_send.at[d, chunk], recv_sem=st_recv.at[me, chunk],
            device_id=peer(d), device_id_type=MESH)

    def wait_stats(chunk):
        for d in range(1, n):
            src = lax.rem(me + d, n)
            part = stats.at[src, pl.ds(chunk * half, half)]
            pltpu.make_async_remote_copy(
                src_ref=part, dst_ref=part, send_sem=st_send.at[d, chunk], recv_sem=st_recv.at[src, chunk],
                device_id=peer(d), device_id_type=MESH).wait_recv()

    gather = RingGather(next_buf, own_v, stage, me, *gather_sems)

    def lay(x):
        return x if len(k_out.shape) == 2 else x.reshape(x.shape[0], heads, HEAD_DIM)

    @pl.when(step == 0)
    def _():
        greet(n, me)
        own_load = pltpu.make_async_copy(gather.block(me), own_v, own_sem)
        own_load.start()
        pl.semaphore_wait(pltpu.get_barrier_semaphore(), n - 1)
        own_load.wait()
        gather.send((0,))

    @pl.when(step == 3)
    def _():
        gather.send((1,))

    @pl.when(step == half)
    def _():
        for d in range(1, n):
            stats_copy(0, d).start()

    @pl.when(step == half + 2)
    def _():
        gather.send((2,))

    @pl.when(step == n)
    def _():
        for d in range(1, n):
            stats_copy(1, d).start()
        gather.send((3,))

    @pl.when(step == 3 * n)
    def _():
        gather.relay()

    @pl.when(step == 3 * n + half)
    def _():
        gather.take((3, 7))

    @pl.when(step < n)
    def _():
        h = h_ref[...]
        q = jnp.dot(h, wq_ref[...], preferred_element_type=jnp.float32).astype(jnp.bfloat16)
        k = jnp.dot(h, wk_ref[...], preferred_element_type=jnp.float32).astype(jnp.bfloat16)
        q_s[step] = q
        k_s[step] = k
        qf, kf = q.astype(jnp.float32), k.astype(jnp.float32)
        q_sq = jnp.sum(qf * qf, axis=1, keepdims=True)
        k_sq = jnp.sum(kf * kf, axis=1, keepdims=True)
        lane = lax.broadcasted_iota(jnp.int32, (HEAD_DIM, HEAD_DIM), 1)
        rows = []
        for g in range(groups):
            part = slice(g * HEAD_DIM, (g + 1) * HEAD_DIM)
            both = jnp.where(lane == 0, q_sq[part], k_sq[part])
            rows.append(both.T[:2])
        stats[me, step] = jnp.concatenate(rows, axis=0)

    @pl.when((step >= n) & (step < 2 * n))
    def _():
        v = jnp.dot(h_ref[...], wv_ref[...], preferred_element_type=jnp.float32).astype(jnp.bfloat16)
        v_out[...] = lay(v)
        vt_s[step - n] = v.T

    @pl.when(step == 2 * n)
    def _():
        wait_stats(0)

    @pl.when(step == 2 * n + half)
    def _():
        wait_stats(1)

    @pl.when((step >= 2 * n) & (step < 3 * n))
    def _():
        j = step - 2 * n
        total = stats[0, j]
        for s in range(1, n):
            total = total + stats[s, j]
        inv = lax.rsqrt(total / width + EPS)
        inv_cols = jnp.concatenate([inv] * (HEAD_DIM // inv.shape[0]), axis=0).T
        for g in range(groups):
            part = slice(g * HEAD_DIM, (g + 1) * HEAD_DIM)
            cos, sin = cos_ref[part, :], sin_ref[part, :]
            for x_s, g_ref, col in ((q_s, qg_ref, 2 * g), (k_s, kg_ref, 2 * g + 1)):
                x = x_s[j, part, :].astype(jnp.float32) * inv_cols[:, col:col + 1] * g_ref[...]
                outs = []
                for hd in range(heads):
                    xh = x[:, hd * HEAD_DIM:(hd + 1) * HEAD_DIM]
                    outs.append((xh * cos + pltpu.roll(xh, HEAD_DIM // 2, 1) * sin).astype(jnp.bfloat16))
                rot = jnp.concatenate(outs, axis=1)
                x_s[j, part, :] = rot
                if x_s is k_s:
                    k_out[part] = lay(rot)

    def o_copy(d):
        return pltpu.make_async_remote_copy(
            src_ref=o_s.at[d], dst_ref=o_hbm.at[:, pl.ds(pl.multiple_of(me * cols, cols), cols)],
            send_sem=o_send.at[d], recv_sem=o_recv.at[me], device_id=peer(d), device_id_type=MESH)

    def o_own():
        return pltpu.make_async_copy(o_s.at[0], o_hbm.at[:, pl.ds(pl.multiple_of(me * cols, cols), cols)], o_local)

    @pl.when(step >= 3 * n)
    def _():
        d = lax.rem(step - 3 * n + 1, n)
        blk = lax.rem(me + d, n)
        scale = HEAD_DIM ** -0.5 * math.log2(math.e)
        nt = (((1,), (1,)), ((), ()))

        def hcols(hd):
            return slice(hd * HEAD_DIM, (hd + 1) * HEAD_DIM)

        qs = [q_s[blk, :, hcols(hd)] for hd in range(heads)]

        def scores(j, hd):
            return lax.dot_general(k_s[j, :, hcols(hd)], qs[hd], nt, preferred_element_type=jnp.float32)

        key_pos = lax.broadcasted_iota(jnp.int32, (tile, tile), 0)
        query_pos = lax.broadcasted_iota(jnp.int32, (tile, tile), 1)
        keep = key_pos <= query_pos
        carry = []
        for hd in range(heads):
            s = jnp.where(keep, scores(blk, hd), -jnp.inf)
            m = jnp.max(s, axis=0, keepdims=True)
            p = jnp.exp2(s * scale - m * scale)
            l = jnp.sum(p, axis=0, keepdims=True)
            acc = jnp.dot(vt_s[blk, hcols(hd), :], p.astype(jnp.bfloat16), preferred_element_type=jnp.float32)
            carry.append((m, l, acc))

        def body(j, carry):
            out = []
            ss = [scores(j, hd) for hd in range(heads)]
            for hd in range(heads):
                m, l, acc = carry[hd]
                s = ss[hd]
                m_new = jnp.maximum(m, jnp.max(s, axis=0, keepdims=True))
                alpha = jnp.exp2((m - m_new) * scale)
                p = jnp.exp2(s * scale - m_new * scale)
                l = l * alpha + jnp.sum(p, axis=0, keepdims=True)
                acc = acc * alpha + jnp.dot(vt_s[j, hcols(hd), :], p.astype(jnp.bfloat16), preferred_element_type=jnp.float32)
                out.append((m_new, l, acc))
            return tuple(out)

        carry = lax.fori_loop(0, blk, body, tuple(carry))
        for hd in range(heads):
            m, l, acc = carry[hd]
            o_s[d, :, hcols(hd)] = (acc / l).T.astype(jnp.bfloat16)

        @pl.when(d != 0)
        def _():
            o_copy(d).start()

        @pl.when(d == 0)
        def _():
            o_own().start()

    @pl.when(step == 4 * n - 1)
    def _():
        gather.finish()
        o_own().wait()
        for d in range(1, n):
            src = lax.rem(me + d, n)
            o_copy(d).wait_send()
            pltpu.make_async_remote_copy(
                src_ref=o_s.at[d], dst_ref=o_hbm.at[:, pl.ds(pl.multiple_of(src * cols, cols), cols)],
                send_sem=o_send.at[d], recv_sem=o_recv.at[src], device_id=peer(d), device_id_type=MESH).wait_recv()
            for chunk in range(2):
                stats_copy(chunk, d).wait_send()


def block_call(n, h_full, wq, wk, wv, qg, kg, cos, sin, next_buf, cached):
    seq, width = h_full.shape
    cols = wq.shape[1]
    tile = seq // n
    heads = cols // HEAD_DIM

    def twice(i):
        return (jnp.where(i < 2 * n, lax.rem(i, n), n - 1), 0)

    def second(i):
        return (jnp.clip(i - n, 0, n - 1), 0)

    def third(i):
        return (jnp.clip(i - 2 * n, 0, n - 1), 0)

    def whole(i):
        return (0, 0)

    cache_tile = (tile, heads, HEAD_DIM) if cached else (tile, cols)
    cache_shape = (seq,) + cache_tile[1:]
    hbm = pl.BlockSpec(memory_space=pl.ANY)

    def cache_map(index):
        return (lambda i: index(i) + (0,)) if cached else index

    flops = 2 * seq * width * cols * 3 + 2 * seq * seq * cols * 2
    return pl.pallas_call(
        functools.partial(block_kernel, n, width),
        grid=(4 * n,),
        in_specs=[
            pl.BlockSpec((tile, width), twice),
            pl.BlockSpec((width, cols), whole), pl.BlockSpec((width, cols), whole), pl.BlockSpec((width, cols), whole),
            pl.BlockSpec((1, cols), whole), pl.BlockSpec((1, cols), whole),
            pl.BlockSpec((tile, HEAD_DIM), third), pl.BlockSpec((tile, HEAD_DIM), third),
            hbm,
        ],
        out_specs=[
            hbm, hbm,
            pl.BlockSpec(cache_tile, cache_map(third)),
            pl.BlockSpec(cache_tile, cache_map(second)),
        ],
        out_shape=[
            jax.ShapeDtypeStruct((tile, n * cols), jnp.bfloat16),
            jax.ShapeDtypeStruct(next_buf.shape, next_buf.dtype),
            jax.ShapeDtypeStruct(cache_shape, jnp.bfloat16),
            jax.ShapeDtypeStruct(cache_shape, jnp.bfloat16),
        ],
        input_output_aliases={8: 1},
        scratch_shapes=[
            pltpu.VMEM((n, tile, cols), jnp.bfloat16),
            pltpu.VMEM((n, tile, cols), jnp.bfloat16),
            pltpu.VMEM((n, cols, tile), jnp.bfloat16),
            pltpu.VMEM((n, n, 2 * tile // HEAD_DIM, HEAD_DIM), jnp.float32),
            pltpu.VMEM((n, tile, cols), jnp.bfloat16),
            pltpu.VMEM((next_buf.shape[0] // n, width), jnp.bfloat16),
            pltpu.VMEM((3, next_buf.shape[0] // n, width), jnp.bfloat16),
            pltpu.SemaphoreType.DMA,
            pltpu.SemaphoreType.DMA((n, 2)),
            pltpu.SemaphoreType.DMA((n, 2)),
            pltpu.SemaphoreType.DMA((n,)),
            pltpu.SemaphoreType.DMA((n,)),
            pltpu.SemaphoreType.DMA,
        ] + GATHER_SEMS,
        compiler_params=pltpu.CompilerParams(
            collective_id=1 if cached else 2, has_side_effects=True, vmem_limit_bytes=52 * 1024 * 1024,
            dimension_semantics=('arbitrary',)),
        cost_estimate=pl.CostEstimate(flops=flops, bytes_accessed=seq * width * 2 + 6 * seq * cols * 2, transcendentals=seq * seq * heads // 2),
        name='attn_block' if cached else 'attn_last',
    )(h_full, wq, wk, wv, qg, kg, cos, sin, next_buf)


N_CHUNK = 4


def last_kernel(n_batch, *refs):
    x_ref, wo_hbm = refs[:2]
    o_hbm = refs[2:2 + n_batch]
    rest = refs[2 + n_batch:]
    caches = rest[:2 * (n_batch - 1)]
    k_last, v_last = rest[2 * (n_batch - 1):2 * n_batch]
    out_ref, k_cache, v_cache = rest[2 * n_batch:2 * n_batch + 3]
    w_v, o_v, c_v, l_v, w_sem, o_sem, ci_sem, co_sem, lo_sem = rest[2 * n_batch + 3:]
    step = pl.program_id(0)
    b, j = step // N_CHUNK, lax.rem(step, N_CHUNK)
    chunk = w_v.shape[2]
    rows = c_v.shape[1]
    per = caches[0].shape[0] // rows
    slots = c_v.shape[0]

    def w_copy(c):
        return pltpu.make_async_copy(wo_hbm.at[:, pl.ds(c * chunk, chunk)], w_v.at[c], w_sem.at[c])

    def o_copy(i):
        return pltpu.make_async_copy(o_hbm[i], o_v.at[i], o_sem.at[i])

    @pl.when(step == 0)
    def _():
        w_copy(0).start()
        o_copy(0).start()
        for c in range(1, N_CHUNK):
            w_copy(c).start()
        for i in range(1, n_batch):
            o_copy(i).start()

    for i in range(n_batch):
        @pl.when(step == i * N_CHUNK)
        def _(i=i):
            o_copy(i).wait()
    for c in range(N_CHUNK):
        @pl.when(step == c)
        def _(c=c):
            w_copy(c).wait()

    items = [(i, part) for i in range(len(caches)) for part in range(per)]

    def item_in(t):
        i, part = items[t]
        return pltpu.make_async_copy(caches[i].at[pl.ds(part * rows, rows)], c_v.at[t % slots], ci_sem.at[t % slots])

    def item_out(t):
        i, part = items[t]
        cache = k_cache if i % 2 == 0 else v_cache
        return pltpu.make_async_copy(c_v.at[t % slots], cache.at[i // 2, pl.ds(part * rows, rows)], co_sem.at[t % slots])

    for t in range(len(items) + slots):
        @pl.when(step == t)
        def _(t=t):
            if t >= slots:
                item_out(t - slots).wait()
            if t < len(items):
                item_in(t).start()
            if 1 <= t <= len(items):
                item_in(t - 1).wait()
                item_out(t - 1).start()

    last_rows = l_v.shape[2]

    def last_out(which, t):
        cache = (k_cache, v_cache)[which]
        return pltpu.make_async_copy(l_v.at[which, lax.rem(t, 2)],
                                     cache.at[n_batch - 1, pl.ds(pl.multiple_of(t * last_rows, last_rows), last_rows)],
                                     lo_sem.at[which, lax.rem(t, 2)])

    @pl.when(step >= 2)
    def _():
        for which in range(2):
            last_out(which, step - 2).wait()
    for which, src in enumerate((k_last, v_last)):
        l_v[which, lax.rem(step, 2)] = src[...].reshape(l_v.shape[2:])
        last_out(which, step).start()

    y = jnp.dot(o_v[b], w_v[j], preferred_element_type=jnp.float32).astype(jnp.bfloat16)
    out_ref[0] = (x_ref[0].astype(jnp.float32) + y.astype(jnp.float32)).astype(jnp.bfloat16)

    @pl.when(step == n_batch * N_CHUNK - 1)
    def _():
        for which in range(2):
            for back in (1, 0):
                last_out(which, step - back).wait()


def last_call(x_local, w_o, os, ks, vs):
    n_batch, rows, width = x_local.shape
    seq, heads, _ = ks[0].shape
    steps = n_batch * N_CHUNK
    hbm = pl.BlockSpec(memory_space=pl.ANY)
    block = pl.BlockSpec((1, rows, width // N_CHUNK), lambda i: (i // N_CHUNK, 0, lax.rem(i, N_CHUNK)))
    last = pl.BlockSpec((seq // steps, heads * HEAD_DIM), lambda i: (i, 0))
    caches = [c for pair in zip(ks[:-1], vs[:-1]) for c in pair]
    cache = jax.ShapeDtypeStruct((n_batch, seq, heads, HEAD_DIM), jnp.bfloat16)
    return pl.pallas_call(
        functools.partial(last_kernel, n_batch),
        grid=(steps,),
        in_specs=[block, hbm] + [hbm] * (n_batch + len(caches)) + [last, last],
        out_specs=[block, hbm, hbm],
        out_shape=[jax.ShapeDtypeStruct(x_local.shape, jnp.bfloat16), cache, cache],
        scratch_shapes=[
            pltpu.VMEM((N_CHUNK, w_o.shape[0], width // N_CHUNK), jnp.bfloat16),
            pltpu.VMEM((n_batch, rows, w_o.shape[0]), jnp.bfloat16),
            pltpu.VMEM((4, 2048, heads, HEAD_DIM), jnp.bfloat16),
            pltpu.VMEM((2, 2, seq // steps, heads, HEAD_DIM), jnp.bfloat16),
            pltpu.SemaphoreType.DMA((N_CHUNK,)),
            pltpu.SemaphoreType.DMA((n_batch,)),
            pltpu.SemaphoreType.DMA((4,)),
            pltpu.SemaphoreType.DMA((4,)),
            pltpu.SemaphoreType.DMA((2, 2)),
        ],
        compiler_params=pltpu.CompilerParams(
            vmem_limit_bytes=52 * 1024 * 1024, dimension_semantics=('arbitrary',)),
        cost_estimate=pl.CostEstimate(flops=2 * n_batch * rows * width * w_o.shape[0],
                                      bytes_accessed=8 * n_batch * rows * width * 2, transcendentals=0),
        name='last_proj',
    )(x_local, w_o, *os, *caches, ks[-1], vs[-1])


def solution(mesh):
    n = mesh.shape['tp']
    assert n == 8 and tuple(mesh.axis_names) == ('dp', 'tp')

    def local_block(x_local, attn_gain, wq, wk, wv, qg, kg, wo_rows):
        n_batch, rows, width = x_local.shape
        cols = wq.shape[1]
        qg2, kg2 = qg.reshape(1, cols), kg.reshape(1, cols)
        half_dim = HEAD_DIM // 2
        inv_freq = 10000.0 ** (-jnp.arange(half_dim, dtype=jnp.float32) * (2.0 / HEAD_DIM))
        freq = jnp.concatenate([inv_freq, inv_freq]).reshape(1, HEAD_DIM)
        *hs, w_o, cos, sin = first_call(n, x_local, attn_gain.reshape(1, width), wo_rows, freq)
        os, ks, vs = [], [], []
        for b in range(n_batch):
            more = b + 1 < n_batch
            o, gathered, k, v = block_call(n, hs[b], wq, wk, wv, qg2, kg2, cos, sin, hs[b + 1] if more else w_o, more)
            if more:
                hs[b + 1] = gathered
            else:
                w_o = gathered
            os.append(o)
            ks.append(k)
            vs.append(v)
        return tuple(last_call(x_local, w_o, os, ks, vs))

    seq_spec = P('dp', 'tp', None)
    head_spec = P('dp', None, 'tp', None)
    col_spec = P(None, 'tp')
    return jax.shard_map(local_block, mesh=mesh, in_specs=(seq_spec, P(None), col_spec, col_spec, col_spec, P('tp'), P('tp'), P('tp', None)), out_specs=(seq_spec, head_spec, head_spec), check_vma=False)
```

```python
import functools
import math

import jax
import jax.numpy as jnp
from jax import lax
from jax.experimental import pallas as pl
from jax.experimental.pallas import tpu as pltpu
from jax.sharding import PartitionSpec as P

HEAD_DIM = 128
EPS = 1e-5
MESH = pl.DeviceIdType.MESH


FIRST = ((0, 2), (2, 1), (3, 1), (4, 4))
SECOND = ((4, 2), (6, 1), (7, 1), (0, 4))
PIECES = FIRST + SECOND + ((4, 4), (0, 4))
LAST = len(PIECES)


class RingGather:
    def __init__(self, buf, own, stage, me, ici_send, ici_recv, d2d_send, d2d_recv, keep):
        self.buf, self.own, self.stage, self.me, self.rows = buf, own, stage, me, own.shape[0]
        self.ici_send, self.ici_recv, self.d2d_send, self.d2d_recv, self.keep = ici_send, ici_recv, d2d_send, d2d_recv, keep
        self.xn = me + 2 - 4 * lax.rem(me // 2, 2)
        self.yn = me + 4 - 8 * (me // 4)
        self.dg = self.yn + 2 - 4 * lax.rem(me // 2, 2)
        self.pt = me + 1 - 2 * lax.rem(me, 2)

    def block(self, block):
        return self.buf.at[pl.ds(pl.multiple_of(block * self.rows, self.rows), self.rows)]

    def span(self, piece):
        unit = self.rows // 8
        return PIECES[piece][0] * unit, PIECES[piece][1] * unit

    def slot(self, block, piece):
        first, rows = self.span(piece)
        unit = self.rows // 8
        return self.buf.at[pl.ds(pl.multiple_of(block * self.rows + first, unit), rows)]

    def staged(self, piece):
        first, rows = self.span(piece)
        which = 0 if piece < 4 else 1 if piece < 8 else 2
        return self.stage.at[which, pl.ds(first, rows)]

    def source(self, piece):
        return self.xn if piece < 4 else self.yn if piece < 8 else self.dg

    def copy(self, piece):
        first, rows = self.span(piece)
        if piece < 8:
            src = self.own.at[pl.ds(first, rows)]
        else:
            src = self.stage.at[1 if piece == 8 else 0, pl.ds(first, rows)]
        return pltpu.make_async_remote_copy(
            src_ref=src, dst_ref=self.staged(piece), send_sem=self.ici_send.at[piece], recv_sem=self.ici_recv.at[piece],
            device_id={'tp': self.xn if piece < 4 or piece == 8 else self.yn}, device_id_type=MESH)

    def handover(self, piece):
        if piece == LAST:
            src, dst = self.own, self.block(self.me)
        else:
            src, dst = self.staged(piece), self.slot(self.source(piece), piece)
        return pltpu.make_async_remote_copy(
            src_ref=src, dst_ref=dst, send_sem=self.d2d_send.at[piece], recv_sem=self.d2d_recv.at[piece],
            device_id={'tp': self.pt}, device_id_type=MESH)

    def store(self, piece):
        return pltpu.make_async_copy(self.staged(piece), self.slot(self.source(piece), piece), self.keep.at[piece])

    def send(self, turns):
        for turn in turns:
            self.copy(turn).start()
            self.copy(4 + turn).start()
        if 3 in turns:
            self.handover(LAST).start()

    def relay(self):
        for turns, onward in (((0, 1, 2), 9), ((4, 5, 6), 8)):
            for piece in turns:
                self.copy(piece).wait_recv()
            self.copy(onward).start()
        self.pass_on((0, 1, 2, 4, 5, 6))

    def pass_on(self, pieces):
        for piece in pieces:
            self.handover(piece).start()
            self.store(piece).start()

    def take(self, pieces):
        for piece in pieces:
            self.copy(piece).wait_recv()
            self.pass_on((piece,))

    def finish(self):
        self.take((8, 9))
        for piece in range(LAST):
            self.copy(piece).wait_send()
            self.store(piece).wait()
        for piece in range(LAST + 1):
            src = self.pt if piece == LAST else self.pt + self.source(piece) - self.me
            part = self.block(src) if piece == LAST else self.slot(src, piece)
            pltpu.make_async_remote_copy(
                src_ref=part, dst_ref=part, send_sem=self.d2d_send.at[piece], recv_sem=self.d2d_recv.at[piece],
                device_id={'tp': self.pt}, device_id_type=MESH).wait_recv()
            self.handover(piece).wait_send()


GATHER_SEMS = [pltpu.SemaphoreType.DMA((LAST,)), pltpu.SemaphoreType.DMA((LAST,)),
               pltpu.SemaphoreType.DMA((LAST + 1,)), pltpu.SemaphoreType.DMA((LAST + 1,)), pltpu.SemaphoreType.DMA((LAST,))]


def greet(n, me):
    barrier = pltpu.get_barrier_semaphore()
    for d in range(1, n):
        pl.semaphore_signal(barrier, inc=1, device_id={'tp': lax.rem(me + d, n)}, device_id_type=MESH)


def first_kernel(n, n_batch, x_hbm, gain_ref, wo_hbm, freq_ref,
                 h0, h1, h2, h3, wo_full, cos_hbm, sin_hbm,
                 x_v, h_v, wo_v, stage, cos_v, sin_v, in_sem, wo_sem, out_sem, tab_sem, *gather_sems):
    me = lax.axis_index('tp')
    rows, width = x_v.shape[1:]
    wo_rows = wo_v.shape[0]
    hs = (h0, h1, h2, h3)
    greet(n, me)
    loads = [pltpu.make_async_copy(x_hbm.at[b], x_v.at[b], in_sem.at[b]) for b in range(n_batch)]
    wo_load = pltpu.make_async_copy(wo_hbm, wo_v, wo_sem.at[0])
    wo_store = pltpu.make_async_copy(wo_v, wo_full.at[pl.ds(pl.multiple_of(me * wo_rows, wo_rows), wo_rows)], wo_sem.at[1])
    stores = [pltpu.make_async_copy(h_v.at[b], hs[b].at[pl.ds(pl.multiple_of(me * rows, rows), rows)], out_sem.at[b])
              for b in range(n_batch)]
    loads[0].start()

    def norm(b, first=0, strips=rows // 64):
        def body(r, carry):
            part = pl.ds(pl.multiple_of(r * 64, 64), 64)
            x = x_v[b, part, :].astype(jnp.float32)
            inv = lax.rsqrt(jnp.mean(x * x, axis=-1, keepdims=True) + EPS)
            h_v[b, part, :] = (x * inv * gain_ref[...]).astype(jnp.bfloat16)
            return carry
        lax.fori_loop(first, first + strips, body, 0)

    loads[0].wait()
    for load in loads[1:]:
        load.start()
    wo_load.start()
    quarter = rows // 256
    norm(0, 0, quarter)
    norm(0, 2 * quarter, quarter)
    pl.semaphore_wait(pltpu.get_barrier_semaphore(), n - 1)
    gather = RingGather(h0, h_v.at[0], stage, me, *gather_sems)
    gather.send((0,))
    norm(0, quarter, quarter)
    norm(0, 3 * quarter, quarter)
    gather.send((1, 2, 3))
    stores[0].start()
    for b in range(1, n_batch):
        loads[b].wait()
        norm(b)
        stores[b].start()
    wo_load.wait()
    wo_store.start()
    seq = cos_v.shape[0]

    def table(r, carry):
        part = pl.ds(pl.multiple_of(r * 64, 64), 64)
        pos = (lax.broadcasted_iota(jnp.int32, (64, HEAD_DIM), 0) + r * 64).astype(jnp.float32)
        lane = lax.broadcasted_iota(jnp.int32, (64, HEAD_DIM), 1)
        angle = pos * freq_ref[...]
        sin = jnp.sin(angle)
        cos_v[part, :] = jnp.cos(angle)
        sin_v[part, :] = jnp.where(lane < HEAD_DIM // 2, -sin, sin)
        return carry

    lax.fori_loop(0, seq // 64, table, 0)
    tables = [pltpu.make_async_copy(cos_v, cos_hbm, tab_sem.at[0]), pltpu.make_async_copy(sin_v, sin_hbm, tab_sem.at[1])]
    for copy in tables:
        copy.start()
    gather.relay()
    gather.take((3, 7))
    for copy in stores + [wo_store] + tables:
        copy.wait()
    gather.finish()


def first_call(n, x_local, gain, wo_rows, freq):
    n_batch, rows, width = x_local.shape
    depth = wo_rows.shape[0]
    seq = n * rows
    hbm = pl.BlockSpec(memory_space=pl.ANY)
    vmem = pl.BlockSpec(memory_space=pltpu.VMEM)
    return pl.pallas_call(
        functools.partial(first_kernel, n, n_batch),
        in_specs=[hbm, vmem, hbm, vmem],
        out_specs=[hbm] * (n_batch + 3),
        out_shape=[jax.ShapeDtypeStruct((seq, width), jnp.bfloat16)] * n_batch
        + [jax.ShapeDtypeStruct((n * depth, width), jnp.bfloat16)]
        + [jax.ShapeDtypeStruct((seq, HEAD_DIM), jnp.float32)] * 2,
        scratch_shapes=[
            pltpu.VMEM((n_batch, rows, width), jnp.bfloat16),
            pltpu.VMEM((n_batch, rows, width), jnp.bfloat16),
            pltpu.VMEM((depth, width), jnp.bfloat16),
            pltpu.VMEM((3, rows, width), jnp.bfloat16),
            pltpu.VMEM((seq, HEAD_DIM), jnp.float32),
            pltpu.VMEM((seq, HEAD_DIM), jnp.float32),
            pltpu.SemaphoreType.DMA((n_batch,)),
            pltpu.SemaphoreType.DMA((2,)),
            pltpu.SemaphoreType.DMA((n_batch,)),
            pltpu.SemaphoreType.DMA((2,)),
        ] + GATHER_SEMS,
        compiler_params=pltpu.CompilerParams(
            collective_id=0, has_side_effects=True, vmem_limit_bytes=62 * 1024 * 1024),
        cost_estimate=pl.CostEstimate(flops=100000000, bytes_accessed=seq * width * 4, transcendentals=seq * HEAD_DIM * 2),
        name='first_gather',
    )(x_local, gain, wo_rows, freq)


AHEAD = 2


def block_kernel(n, width, h_hbm, wq_hbm, wk_hbm, wv_hbm, qg_ref, kg_ref, cos_hbm, sin_hbm, next_in,
                 o_hbm, next_buf, k_out, v_out,
                 h_v, wqk_v, wv_v, cos_v, sin_v, q_s, k_s, vt_s, k_st, v_st, stats, o_s, s_buf, p_buf, acc_buf, own_v, stage,
                 h_sem, w_sem, tab_sem, kv_sem, own_sem, st_send, st_recv, o_send, o_recv, o_local, *gather_sems):
    me = lax.axis_index('tp')
    tile = h_v.shape[1]
    cols = wv_v.shape[1]
    heads = cols // HEAD_DIM
    groups = tile // HEAD_DIM
    half = n // 2
    gather = RingGather(next_buf, own_v, stage, me, *gather_sems)
    scale = HEAD_DIM ** -0.5 * math.log2(math.e)

    def peer(d):
        return {'tp': lax.rem(me + d, n)}

    def stats_copy(chunk, d):
        part = stats.at[me, pl.ds(chunk * half, half)]
        return pltpu.make_async_remote_copy(
            src_ref=part, dst_ref=part, send_sem=st_send.at[d, chunk], recv_sem=st_recv.at[me, chunk],
            device_id=peer(d), device_id_type=MESH)

    def send_stats(chunk):
        for d in range(1, n):
            stats_copy(chunk, d).start()

    def wait_stats(chunk):
        for d in range(1, n):
            src = lax.rem(me + d, n)
            part = stats.at[src, pl.ds(chunk * half, half)]
            pltpu.make_async_remote_copy(
                src_ref=part, dst_ref=part, send_sem=st_send.at[d, chunk], recv_sem=st_recv.at[src, chunk],
                device_id=peer(d), device_id_type=MESH).wait_recv()

    def lay(x):
        return x if len(k_out.shape) == 2 else x.reshape(x.shape[0], heads, HEAD_DIM)

    def hcols(hd):
        return slice(hd * HEAD_DIM, (hd + 1) * HEAD_DIM)

    def rows_of(i):
        return pl.ds(pl.multiple_of(i * tile, tile), tile)

    def h_load(i):
        return pltpu.make_async_copy(h_hbm.at[rows_of(i)], h_v.at[i], h_sem.at[i])

    def kv_store(which, i):
        src, dst = ((k_st, k_out), (v_st, v_out))[which]
        return pltpu.make_async_copy(src.at[i], dst.at[rows_of(i)], kv_sem.at[which, i])

    w_loads = [
        pltpu.make_async_copy(wq_hbm, wqk_v.at[:, pl.ds(0, cols)], w_sem.at[0]),
        pltpu.make_async_copy(wk_hbm, wqk_v.at[:, pl.ds(cols, cols)], w_sem.at[1]),
        pltpu.make_async_copy(wv_hbm, wv_v, w_sem.at[2])]
    tab_loads = [pltpu.make_async_copy(cos_hbm, cos_v, tab_sem.at[0]), pltpu.make_async_copy(sin_hbm, sin_v, tab_sem.at[1])]
    own_load = pltpu.make_async_copy(gather.block(me), own_v, own_sem)

    greet(n, me)
    own_load.start()
    for load in w_loads[:2] + [h_load(i) for i in range(AHEAD)] + w_loads[2:]:
        load.start()
    own_load.wait()
    pl.semaphore_wait(pltpu.get_barrier_semaphore(), n - 1)
    gather.send((0,))
    for load in w_loads[:2]:
        load.wait()

    def qk_block(i, carry):
        @pl.when(i + AHEAD < n)
        def _():
            h_load(i + AHEAD).start()

        h_load(i).wait()
        qk = jnp.dot(h_v[i], wqk_v[...], preferred_element_type=jnp.float32).astype(jnp.bfloat16)
        q, k = qk[:, :cols], qk[:, cols:]
        q_s[i] = q
        k_s[i] = k
        qf, kf = q.astype(jnp.float32), k.astype(jnp.float32)
        q_sq = jnp.sum(qf * qf, axis=1, keepdims=True)
        k_sq = jnp.sum(kf * kf, axis=1, keepdims=True)
        lane = lax.broadcasted_iota(jnp.int32, (HEAD_DIM, HEAD_DIM), 1)
        rows = []
        for g in range(groups):
            part = slice(g * HEAD_DIM, (g + 1) * HEAD_DIM)
            both = jnp.where(lane == 0, q_sq[part], k_sq[part])
            rows.append(both.T[:2])
        stats[me, i] = jnp.concatenate(rows, axis=0)
        return carry

    lax.fori_loop(0, half, qk_block, 0)
    for load in tab_loads:
        load.start()
    send_stats(0)
    gather.send((1,))
    lax.fori_loop(half, n, qk_block, 0)
    send_stats(1)
    gather.send((2, 3))
    w_loads[2].wait()

    def v_block(i, carry):
        v = jnp.dot(h_v[i], wv_v[...], preferred_element_type=jnp.float32).astype(jnp.bfloat16)
        v_st[i] = lay(v)
        kv_store(1, i).start()
        vt_s[i] = v.T
        return carry

    lax.fori_loop(0, n, v_block, 0)
    for load in tab_loads:
        load.wait()

    def norm_block(j, carry):
        total = stats[0, j]
        for src in range(1, n):
            total = total + stats[src, j]
        inv = lax.rsqrt(total / width + EPS)
        inv_cols = jnp.concatenate([inv] * (HEAD_DIM // inv.shape[0]), axis=0).T
        for g in range(groups):
            part = slice(g * HEAD_DIM, (g + 1) * HEAD_DIM)
            tab = pl.ds(pl.multiple_of(j * tile + g * HEAD_DIM, HEAD_DIM), HEAD_DIM)
            cos, sin = cos_v[tab, :], sin_v[tab, :]
            for x_s, g_ref, col in ((q_s, qg_ref, 2 * g), (k_s, kg_ref, 2 * g + 1)):
                x = x_s[j, part, :].astype(jnp.float32) * inv_cols[:, col:col + 1] * g_ref[...]
                outs = []
                for hd in range(heads):
                    xh = x[:, hcols(hd)]
                    outs.append((xh * cos + pltpu.roll(xh, HEAD_DIM // 2, 1) * sin).astype(jnp.bfloat16))
                rot = jnp.concatenate(outs, axis=1)
                x_s[j, part, :] = rot
                if x_s is k_s:
                    k_st[j, part] = lay(rot)
        kv_store(0, j).start()
        return carry

    wait_stats(0)
    lax.fori_loop(0, half, norm_block, 0)
    wait_stats(1)
    lax.fori_loop(half, n, norm_block, 0)

    def o_copy(d):
        return pltpu.make_async_remote_copy(
            src_ref=o_s.at[d], dst_ref=o_hbm.at[:, pl.ds(pl.multiple_of(me * cols, cols), cols)],
            send_sem=o_send.at[d], recv_sem=o_recv.at[me], device_id=peer(d), device_id_type=MESH)

    def o_own():
        return pltpu.make_async_copy(o_s.at[0], o_hbm.at[:, pl.ds(pl.multiple_of(me * cols, cols), cols)], o_local)

    nt = (((1,), (1,)), ((), ()))
    strip = 64

    def softmax_step(j, hd, m, l):
        top = None
        for c in range(tile // strip):
            part = jnp.max(s_buf[hd, c * strip:(c + 1) * strip, :].reshape(strip // 8, 8, tile), axis=0)
            top = part if top is None else jnp.maximum(top, part)
        m_new = jnp.max(top, axis=0, keepdims=True)
        if m is not None:
            m_new = jnp.maximum(m, m_new)
        m_scaled = m_new * scale
        total = None
        for c in range(tile // strip):
            p = jnp.exp2(s_buf[hd, c * strip:(c + 1) * strip, :] * scale - m_scaled)
            part = jnp.sum(p.reshape(strip // 8, 8, tile), axis=0)
            total = part if total is None else total + part
            p_buf[hd, c * strip:(c + 1) * strip, :] = p.astype(jnp.bfloat16)
        l_new = jnp.sum(total, axis=0, keepdims=True)
        pv = jnp.dot(vt_s[j, hcols(hd), :], p_buf[hd], preferred_element_type=jnp.float32)
        if m is None:
            acc_buf[hd] = pv
        else:
            alpha = jnp.exp2((m - m_new) * scale)
            l_new = l * alpha + l_new
            acc_buf[hd] = acc_buf[hd] * alpha + pv
        return m_new, l_new

    def attend(step, carry):
        d = lax.rem(step + 1, n)
        blk = lax.rem(me + d, n)

        def scores(j, hd):
            return lax.dot_general(k_s[j, :, hcols(hd)], q_s[blk, :, hcols(hd)], nt, preferred_element_type=jnp.float32)

        keep = lax.broadcasted_iota(jnp.int32, (tile, tile), 0) <= lax.broadcasted_iota(jnp.int32, (tile, tile), 1)
        for hd in range(heads):
            s_buf[hd] = jnp.where(keep, scores(blk, hd), -jnp.inf)
        state = tuple(softmax_step(blk, hd, None, None) for hd in range(heads))

        def body(j, state):
            for hd in range(heads):
                s_buf[hd] = scores(j, hd)
            return tuple(softmax_step(j, hd, *state[hd]) for hd in range(heads))

        state = lax.fori_loop(0, blk, body, state)
        for hd in range(heads):
            o_s[d, :, hcols(hd)] = (acc_buf[hd] / state[hd][1]).T.astype(jnp.bfloat16)

        @pl.when(d != 0)
        def _():
            o_copy(d).start()

        @pl.when(d == 0)
        def _():
            o_own().start()
        return carry

    gather.relay()
    lax.fori_loop(0, half, attend, 0)
    gather.take((3, 7))
    lax.fori_loop(half, n, attend, 0)
    gather.finish()
    o_own().wait()
    for d in range(1, n):
        src = lax.rem(me + d, n)
        o_copy(d).wait_send()
        pltpu.make_async_remote_copy(
            src_ref=o_s.at[d], dst_ref=o_hbm.at[:, pl.ds(pl.multiple_of(src * cols, cols), cols)],
            send_sem=o_send.at[d], recv_sem=o_recv.at[src], device_id=peer(d), device_id_type=MESH).wait_recv()
        for chunk in range(2):
            stats_copy(chunk, d).wait_send()
    for i in range(n):
        for which in range(2):
            kv_store(which, i).wait()


def block_call(n, h_full, wq, wk, wv, qg, kg, cos, sin, next_buf, cached):
    seq, width = h_full.shape
    cols = wq.shape[1]
    tile = seq // n
    heads = cols // HEAD_DIM
    next_rows = next_buf.shape[0] // n
    cache_tail = (heads, HEAD_DIM) if cached else (cols,)
    hbm = pl.BlockSpec(memory_space=pl.ANY)
    vmem = pl.BlockSpec(memory_space=pltpu.VMEM)
    flops = 2 * seq * width * cols * 3 + 2 * seq * seq * cols * 2
    cache = jax.ShapeDtypeStruct((seq,) + cache_tail, jnp.bfloat16)
    return pl.pallas_call(
        functools.partial(block_kernel, n, width),
        in_specs=[hbm, hbm, hbm, hbm, vmem, vmem, hbm, hbm, hbm],
        out_specs=[hbm, hbm, hbm, hbm],
        out_shape=[
            jax.ShapeDtypeStruct((tile, n * cols), jnp.bfloat16),
            jax.ShapeDtypeStruct(next_buf.shape, next_buf.dtype),
            cache, cache,
        ],
        input_output_aliases={8: 1},
        scratch_shapes=[
            pltpu.VMEM((n, tile, width), jnp.bfloat16),
            pltpu.VMEM((width, 2 * cols), jnp.bfloat16),
            pltpu.VMEM((width, cols), jnp.bfloat16),
            pltpu.VMEM((seq, HEAD_DIM), jnp.float32),
            pltpu.VMEM((seq, HEAD_DIM), jnp.float32),
            pltpu.VMEM((n, tile, cols), jnp.bfloat16),
            pltpu.VMEM((n, tile, cols), jnp.bfloat16),
            pltpu.VMEM((n, cols, tile), jnp.bfloat16),
            pltpu.VMEM((n, tile) + cache_tail, jnp.bfloat16),
            pltpu.VMEM((n, tile) + cache_tail, jnp.bfloat16),
            pltpu.VMEM((n, n, 2 * tile // HEAD_DIM, HEAD_DIM), jnp.float32),
            pltpu.VMEM((n, tile, cols), jnp.bfloat16),
            pltpu.VMEM((heads, tile, tile), jnp.float32),
            pltpu.VMEM((heads, tile, tile), jnp.bfloat16),
            pltpu.VMEM((heads, HEAD_DIM, tile), jnp.float32),
            pltpu.VMEM((next_rows, width), jnp.bfloat16),
            pltpu.VMEM((3, next_rows, width), jnp.bfloat16),
            pltpu.SemaphoreType.DMA((n,)),
            pltpu.SemaphoreType.DMA((3,)),
            pltpu.SemaphoreType.DMA((2,)),
            pltpu.SemaphoreType.DMA((2, n)),
            pltpu.SemaphoreType.DMA,
            pltpu.SemaphoreType.DMA((n, 2)),
            pltpu.SemaphoreType.DMA((n, 2)),
            pltpu.SemaphoreType.DMA((n,)),
            pltpu.SemaphoreType.DMA((n,)),
            pltpu.SemaphoreType.DMA,
        ] + GATHER_SEMS,
        compiler_params=pltpu.CompilerParams(
            collective_id=1 if cached else 2, has_side_effects=True, vmem_limit_bytes=62 * 1024 * 1024),
        cost_estimate=pl.CostEstimate(flops=flops, bytes_accessed=seq * width * 2 + 6 * seq * cols * 2, transcendentals=seq * seq * heads // 2),
        name='attn_block' if cached else 'attn_last',
    )(h_full, wq, wk, wv, qg, kg, cos, sin, next_buf)


N_CHUNK = 4


def last_kernel(n_batch, *refs):
    x_ref, wo_hbm = refs[:2]
    o_hbm = refs[2:2 + n_batch]
    rest = refs[2 + n_batch:]
    caches = rest[:2 * (n_batch - 1)]
    k_last, v_last = rest[2 * (n_batch - 1):2 * n_batch]
    out_ref, k_cache, v_cache = rest[2 * n_batch:2 * n_batch + 3]
    w_v, o_v, c_v, l_v, w_sem, o_sem, ci_sem, co_sem, lo_sem = rest[2 * n_batch + 3:]
    step = pl.program_id(0)
    b, j = step // N_CHUNK, lax.rem(step, N_CHUNK)
    chunk = w_v.shape[2]
    rows = c_v.shape[1]
    per = caches[0].shape[0] // rows
    slots = c_v.shape[0]

    def w_copy(c):
        return pltpu.make_async_copy(wo_hbm.at[:, pl.ds(c * chunk, chunk)], w_v.at[c], w_sem.at[c])

    def o_copy(i):
        return pltpu.make_async_copy(o_hbm[i], o_v.at[i], o_sem.at[i])

    @pl.when(step == 0)
    def _():
        w_copy(0).start()
        o_copy(0).start()
        for c in range(1, N_CHUNK):
            w_copy(c).start()
        for i in range(1, n_batch):
            o_copy(i).start()

    for i in range(n_batch):
        @pl.when(step == i * N_CHUNK)
        def _(i=i):
            o_copy(i).wait()
    for c in range(N_CHUNK):
        @pl.when(step == c)
        def _(c=c):
            w_copy(c).wait()

    items = [(i, part) for i in range(len(caches)) for part in range(per)]

    def item_in(t):
        i, part = items[t]
        return pltpu.make_async_copy(caches[i].at[pl.ds(part * rows, rows)], c_v.at[t % slots], ci_sem.at[t % slots])

    def item_out(t):
        i, part = items[t]
        cache = k_cache if i % 2 == 0 else v_cache
        return pltpu.make_async_copy(c_v.at[t % slots], cache.at[i // 2, pl.ds(part * rows, rows)], co_sem.at[t % slots])

    for t in range(len(items) + slots):
        @pl.when(step == t)
        def _(t=t):
            if t >= slots:
                item_out(t - slots).wait()
            if t < len(items):
                item_in(t).start()
            if 1 <= t <= len(items):
                item_in(t - 1).wait()
                item_out(t - 1).start()

    last_rows = l_v.shape[2]

    def last_out(which, t):
        cache = (k_cache, v_cache)[which]
        return pltpu.make_async_copy(l_v.at[which, lax.rem(t, 2)],
                                     cache.at[n_batch - 1, pl.ds(pl.multiple_of(t * last_rows, last_rows), last_rows)],
                                     lo_sem.at[which, lax.rem(t, 2)])

    @pl.when(step >= 2)
    def _():
        for which in range(2):
            last_out(which, step - 2).wait()
    for which, src in enumerate((k_last, v_last)):
        l_v[which, lax.rem(step, 2)] = src[...].reshape(l_v.shape[2:])
        last_out(which, step).start()

    y = jnp.dot(o_v[b], w_v[j], preferred_element_type=jnp.float32).astype(jnp.bfloat16)
    out_ref[0] = (x_ref[0].astype(jnp.float32) + y.astype(jnp.float32)).astype(jnp.bfloat16)

    @pl.when(step == n_batch * N_CHUNK - 1)
    def _():
        for which in range(2):
            for back in (1, 0):
                last_out(which, step - back).wait()


def last_call(x_local, w_o, os, ks, vs):
    n_batch, rows, width = x_local.shape
    seq, heads, _ = ks[0].shape
    steps = n_batch * N_CHUNK
    hbm = pl.BlockSpec(memory_space=pl.ANY)
    block = pl.BlockSpec((1, rows, width // N_CHUNK), lambda i: (i // N_CHUNK, 0, lax.rem(i, N_CHUNK)))
    last = pl.BlockSpec((seq // steps, heads * HEAD_DIM), lambda i: (i, 0))
    caches = [c for pair in zip(ks[:-1], vs[:-1]) for c in pair]
    cache = jax.ShapeDtypeStruct((n_batch, seq, heads, HEAD_DIM), jnp.bfloat16)
    return pl.pallas_call(
        functools.partial(last_kernel, n_batch),
        grid=(steps,),
        in_specs=[block, hbm] + [hbm] * (n_batch + len(caches)) + [last, last],
        out_specs=[block, hbm, hbm],
        out_shape=[jax.ShapeDtypeStruct(x_local.shape, jnp.bfloat16), cache, cache],
        scratch_shapes=[
            pltpu.VMEM((N_CHUNK, w_o.shape[0], width // N_CHUNK), jnp.bfloat16),
            pltpu.VMEM((n_batch, rows, w_o.shape[0]), jnp.bfloat16),
            pltpu.VMEM((4, 2048, heads, HEAD_DIM), jnp.bfloat16),
            pltpu.VMEM((2, 2, seq // steps, heads, HEAD_DIM), jnp.bfloat16),
            pltpu.SemaphoreType.DMA((N_CHUNK,)),
            pltpu.SemaphoreType.DMA((n_batch,)),
            pltpu.SemaphoreType.DMA((4,)),
            pltpu.SemaphoreType.DMA((4,)),
            pltpu.SemaphoreType.DMA((2, 2)),
        ],
        compiler_params=pltpu.CompilerParams(
            vmem_limit_bytes=52 * 1024 * 1024, dimension_semantics=('arbitrary',)),
        cost_estimate=pl.CostEstimate(flops=2 * n_batch * rows * width * w_o.shape[0],
                                      bytes_accessed=8 * n_batch * rows * width * 2, transcendentals=0),
        name='last_proj',
    )(x_local, w_o, *os, *caches, ks[-1], vs[-1])


def solution(mesh):
    n = mesh.shape['tp']
    assert n == 8 and tuple(mesh.axis_names) == ('dp', 'tp')

    def local_block(x_local, attn_gain, wq, wk, wv, qg, kg, wo_rows):
        n_batch, rows, width = x_local.shape
        cols = wq.shape[1]
        qg2, kg2 = qg.reshape(1, cols), kg.reshape(1, cols)
        half_dim = HEAD_DIM // 2
        inv_freq = 10000.0 ** (-jnp.arange(half_dim, dtype=jnp.float32) * (2.0 / HEAD_DIM))
        freq = jnp.concatenate([inv_freq, inv_freq]).reshape(1, HEAD_DIM)
        *hs, w_o, cos, sin = first_call(n, x_local, attn_gain.reshape(1, width), wo_rows, freq)
        os, ks, vs = [], [], []
        for b in range(n_batch):
            more = b + 1 < n_batch
            o, gathered, k, v = block_call(n, hs[b], wq, wk, wv, qg2, kg2, cos, sin, hs[b + 1] if more else w_o, more)
            if more:
                hs[b + 1] = gathered
            else:
                w_o = gathered
            os.append(o)
            ks.append(k)
            vs.append(v)
        return tuple(last_call(x_local, w_o, os, ks, vs))

    seq_spec = P('dp', 'tp', None)
    head_spec = P('dp', None, 'tp', None)
    col_spec = P(None, 'tp')
    return jax.shard_map(local_block, mesh=mesh, in_specs=(seq_spec, P(None), col_spec, col_spec, col_spec, P('tp'), P('tp'), P('tp', None)), out_specs=(seq_spec, head_spec, head_spec), check_vma=False)
```

```python
import functools
import math

import jax
import jax.numpy as jnp
from jax import lax
from jax.experimental import pallas as pl
from jax.experimental.pallas import tpu as pltpu
from jax.sharding import PartitionSpec as P

HEAD_DIM = 128
EPS = 1e-5
MESH = pl.DeviceIdType.MESH


FIRST = ((0, 2), (2, 1), (3, 1), (4, 4))
SECOND = ((4, 2), (6, 1), (7, 1), (0, 4))
PIECES = FIRST + SECOND + ((4, 2), (6, 2), (0, 2), (2, 2))
LAST = len(PIECES)


class RingGather:
    def __init__(self, buf, own, stage, me, ici_send, ici_recv, d2d_send, d2d_recv, keep):
        self.buf, self.own, self.stage, self.me, self.rows = buf, own, stage, me, stage.shape[1]
        self.ici_send, self.ici_recv, self.d2d_send, self.d2d_recv, self.keep = ici_send, ici_recv, d2d_send, d2d_recv, keep
        self.xn = me + 2 - 4 * lax.rem(me // 2, 2)
        self.yn = me + 4 - 8 * (me // 4)
        self.dg = self.yn + 2 - 4 * lax.rem(me // 2, 2)
        self.pt = me + 1 - 2 * lax.rem(me, 2)

    def block(self, block):
        return self.buf.at[pl.ds(pl.multiple_of(block * self.rows, self.rows), self.rows)]

    def span(self, piece):
        unit = self.rows // 8
        return PIECES[piece][0] * unit, PIECES[piece][1] * unit

    def slot(self, block, piece):
        first, rows = self.span(piece)
        unit = self.rows // 8
        return self.buf.at[pl.ds(pl.multiple_of(block * self.rows + first, unit), rows)]

    def staged(self, piece):
        first, rows = self.span(piece)
        which = 0 if piece < 4 else 1 if piece < 8 else 2
        return self.stage.at[which, pl.ds(first, rows)]

    def source(self, piece):
        return self.xn if piece < 4 else self.yn if piece < 8 else self.dg

    def copy(self, piece):
        first, rows = self.span(piece)
        if piece < 8:
            src = self.slot(self.me, piece) if self.own is None else self.own.at[pl.ds(first, rows)]
        else:
            src = self.stage.at[1 if piece < 10 else 0, pl.ds(first, rows)]
        return pltpu.make_async_remote_copy(
            src_ref=src, dst_ref=self.staged(piece), send_sem=self.ici_send.at[piece], recv_sem=self.ici_recv.at[piece],
            device_id={'tp': self.xn if piece < 4 or piece in (8, 9) else self.yn}, device_id_type=MESH)

    def handover(self, piece):
        if piece == LAST:
            dst = self.block(self.me)
            src = dst if self.own is None else self.own
        else:
            src, dst = self.staged(piece), self.slot(self.source(piece), piece)
        return pltpu.make_async_remote_copy(
            src_ref=src, dst_ref=dst, send_sem=self.d2d_send.at[piece], recv_sem=self.d2d_recv.at[piece],
            device_id={'tp': self.pt}, device_id_type=MESH)

    def store(self, piece):
        return pltpu.make_async_copy(self.staged(piece), self.slot(self.source(piece), piece), self.keep.at[piece])

    def send(self, turns):
        for turn in turns:
            self.copy(turn).start()
            self.copy(4 + turn).start()
        if 3 in turns:
            self.handover(LAST).start()

    def relay(self):
        for turns, onward in (((0,), 10), ((4,), 8), ((1, 2), 11), ((5, 6), 9)):
            for piece in turns:
                self.copy(piece).wait_recv()
            self.copy(onward).start()
        self.pass_on((0, 1, 2, 4, 5, 6))

    def pass_on(self, pieces):
        for piece in pieces:
            self.handover(piece).start()
            self.store(piece).start()

    def take(self, pieces):
        for piece in pieces:
            self.copy(piece).wait_recv()
            self.pass_on((piece,))

    def finish(self):
        self.take((8, 10, 9, 11))
        for piece in range(LAST):
            self.copy(piece).wait_send()
            self.store(piece).wait()
        for piece in range(LAST + 1):
            src = self.pt if piece == LAST else self.pt + self.source(piece) - self.me
            part = self.block(src) if piece == LAST else self.slot(src, piece)
            pltpu.make_async_remote_copy(
                src_ref=part, dst_ref=part, send_sem=self.d2d_send.at[piece], recv_sem=self.d2d_recv.at[piece],
                device_id={'tp': self.pt}, device_id_type=MESH).wait_recv()
            self.handover(piece).wait_send()


GATHER_SEMS = [pltpu.SemaphoreType.DMA((LAST,)), pltpu.SemaphoreType.DMA((LAST,)),
               pltpu.SemaphoreType.DMA((LAST + 1,)), pltpu.SemaphoreType.DMA((LAST + 1,)), pltpu.SemaphoreType.DMA((LAST,))]


def greet(n, me):
    barrier = pltpu.get_barrier_semaphore()
    for d in range(1, n):
        pl.semaphore_signal(barrier, inc=1, device_id={'tp': lax.rem(me + d, n)}, device_id_type=MESH)


def first_kernel(n, n_batch, x_hbm, gain_ref, wo_hbm, freq_ref,
                 h0, h1, h2, h3, wo_full, cos_hbm, sin_hbm,
                 x_v, h_v, wo_v, stage, cos_v, sin_v, in_sem, wo_sem, out_sem, tab_sem, *gather_sems):
    me = lax.axis_index('tp')
    rows, width = x_v.shape[1:]
    wo_rows = wo_v.shape[0]
    hs = (h0, h1, h2, h3)
    greet(n, me)
    loads = [pltpu.make_async_copy(x_hbm.at[b], x_v.at[b], in_sem.at[b]) for b in range(n_batch)]
    wo_load = pltpu.make_async_copy(wo_hbm, wo_v, wo_sem.at[0])
    wo_store = pltpu.make_async_copy(wo_v, wo_full.at[pl.ds(pl.multiple_of(me * wo_rows, wo_rows), wo_rows)], wo_sem.at[1])
    stores = [pltpu.make_async_copy(h_v.at[b], hs[b].at[pl.ds(pl.multiple_of(me * rows, rows), rows)], out_sem.at[b])
              for b in range(n_batch)]
    loads[0].start()

    def norm(b, first=0, strips=rows // 64):
        def body(r, carry):
            part = pl.ds(pl.multiple_of(r * 64, 64), 64)
            x = x_v[b, part, :].astype(jnp.float32)
            inv = lax.rsqrt(jnp.mean(x * x, axis=-1, keepdims=True) + EPS)
            h_v[b, part, :] = (x * inv * gain_ref[...]).astype(jnp.bfloat16)
            return carry
        lax.fori_loop(first, first + strips, body, 0)

    loads[0].wait()
    for load in loads[1:]:
        load.start()
    wo_load.start()
    quarter = rows // 256
    norm(0, 0, quarter)
    norm(0, 2 * quarter, quarter)
    pl.semaphore_wait(pltpu.get_barrier_semaphore(), n - 1)
    gather = RingGather(h0, h_v.at[0], stage, me, *gather_sems)
    gather.send((0,))
    norm(0, quarter, quarter)
    norm(0, 3 * quarter, quarter)
    gather.send((1, 2, 3))
    stores[0].start()
    for b in range(1, n_batch):
        loads[b].wait()
        norm(b)
        stores[b].start()
    wo_load.wait()
    wo_store.start()
    seq = cos_v.shape[0]

    def table(r, carry):
        part = pl.ds(pl.multiple_of(r * 64, 64), 64)
        pos = (lax.broadcasted_iota(jnp.int32, (64, HEAD_DIM), 0) + r * 64).astype(jnp.float32)
        lane = lax.broadcasted_iota(jnp.int32, (64, HEAD_DIM), 1)
        angle = pos * freq_ref[...]
        sin = jnp.sin(angle)
        cos_v[part, :] = jnp.cos(angle)
        sin_v[part, :] = jnp.where(lane < HEAD_DIM // 2, -sin, sin)
        return carry

    lax.fori_loop(0, seq // 64, table, 0)
    tables = [pltpu.make_async_copy(cos_v, cos_hbm, tab_sem.at[0]), pltpu.make_async_copy(sin_v, sin_hbm, tab_sem.at[1])]
    for copy in tables:
        copy.start()
    gather.relay()
    gather.take((3, 7))
    for copy in stores + [wo_store] + tables:
        copy.wait()
    gather.finish()


def first_call(n, x_local, gain, wo_rows, freq):
    n_batch, rows, width = x_local.shape
    depth = wo_rows.shape[0]
    seq = n * rows
    hbm = pl.BlockSpec(memory_space=pl.ANY)
    vmem = pl.BlockSpec(memory_space=pltpu.VMEM)
    return pl.pallas_call(
        functools.partial(first_kernel, n, n_batch),
        in_specs=[hbm, vmem, hbm, vmem],
        out_specs=[hbm] * (n_batch + 3),
        out_shape=[jax.ShapeDtypeStruct((seq, width), jnp.bfloat16)] * n_batch
        + [jax.ShapeDtypeStruct((n * depth, width), jnp.bfloat16)]
        + [jax.ShapeDtypeStruct((seq, HEAD_DIM), jnp.float32)] * 2,
        scratch_shapes=[
            pltpu.VMEM((n_batch, rows, width), jnp.bfloat16),
            pltpu.VMEM((n_batch, rows, width), jnp.bfloat16),
            pltpu.VMEM((depth, width), jnp.bfloat16),
            pltpu.VMEM((3, rows, width), jnp.bfloat16),
            pltpu.VMEM((seq, HEAD_DIM), jnp.float32),
            pltpu.VMEM((seq, HEAD_DIM), jnp.float32),
            pltpu.SemaphoreType.DMA((n_batch,)),
            pltpu.SemaphoreType.DMA((2,)),
            pltpu.SemaphoreType.DMA((n_batch,)),
            pltpu.SemaphoreType.DMA((2,)),
        ] + GATHER_SEMS,
        compiler_params=pltpu.CompilerParams(
            collective_id=0, has_side_effects=True, vmem_limit_bytes=62 * 1024 * 1024),
        cost_estimate=pl.CostEstimate(flops=100000000, bytes_accessed=seq * width * 4, transcendentals=seq * HEAD_DIM * 2),
        name='first_gather',
    )(x_local, gain, wo_rows, freq)


AHEAD = 2
SPLIT = 2


def block_kernel(n, width, h_hbm, wq_hbm, wk_hbm, wv_hbm, qg_ref, kg_ref, cos_hbm, sin_hbm, next_in,
                 o_hbm, next_buf, k_out, v_out,
                 h_v, wqk_v, wv_v, cos_v, sin_v, q_s, k_s, vt_s, k_st, v_st, stats, o_s, s_buf, p_buf, acc_buf, stage,
                 h_sem, w_sem, tab_sem, kv_sem, st_send, st_recv, o_send, o_recv, o_local, *gather_sems):
    me = lax.axis_index('tp')
    tile = h_v.shape[1]
    cols = wv_v.shape[1]
    heads = cols // HEAD_DIM
    groups = tile // HEAD_DIM
    half = n // 2
    gather = RingGather(next_buf, None, stage, me, *gather_sems)
    scale = HEAD_DIM ** -0.5 * math.log2(math.e)

    def peer(d):
        return {'tp': lax.rem(me + d, n)}

    def stats_copy(chunk, d):
        part = stats.at[me, pl.ds(chunk * half, half)]
        return pltpu.make_async_remote_copy(
            src_ref=part, dst_ref=part, send_sem=st_send.at[d, chunk], recv_sem=st_recv.at[me, chunk],
            device_id=peer(d), device_id_type=MESH)

    def send_stats(chunk):
        for d in range(1, n):
            stats_copy(chunk, d).start()

    def wait_stats(chunk):
        for d in range(1, n):
            src = lax.rem(me + d, n)
            part = stats.at[src, pl.ds(chunk * half, half)]
            pltpu.make_async_remote_copy(
                src_ref=part, dst_ref=part, send_sem=st_send.at[d, chunk], recv_sem=st_recv.at[src, chunk],
                device_id=peer(d), device_id_type=MESH).wait_recv()

    def lay(x):
        return x if len(k_out.shape) == 2 else x.reshape(x.shape[0], heads, HEAD_DIM)

    def hcols(hd):
        return slice(hd * HEAD_DIM, (hd + 1) * HEAD_DIM)

    def rows_of(i):
        return pl.ds(pl.multiple_of(i * tile, tile), tile)

    def h_load(i):
        return pltpu.make_async_copy(h_hbm.at[rows_of(i)], h_v.at[i], h_sem.at[i])

    def kv_store(which, i):
        src, dst = ((k_st, k_out), (v_st, v_out))[which]
        return pltpu.make_async_copy(src.at[i], dst.at[rows_of(i)], kv_sem.at[which, i])

    w_loads = [
        pltpu.make_async_copy(wq_hbm, wqk_v.at[:, pl.ds(0, cols)], w_sem.at[0]),
        pltpu.make_async_copy(wk_hbm, wqk_v.at[:, pl.ds(cols, cols)], w_sem.at[1]),
        pltpu.make_async_copy(wv_hbm, wv_v, w_sem.at[2])]
    tab_loads = [pltpu.make_async_copy(cos_hbm, cos_v, tab_sem.at[0]), pltpu.make_async_copy(sin_hbm, sin_v, tab_sem.at[1])]

    greet(n, me)
    for load in w_loads[:2] + [h_load(i) for i in range(AHEAD)] + w_loads[2:]:
        load.start()
    pl.semaphore_wait(pltpu.get_barrier_semaphore(), n - 1)
    gather.send((0,))
    for load in w_loads[:2]:
        load.wait()

    def qk_block(i, carry):
        @pl.when(i + AHEAD < n)
        def _():
            h_load(i + AHEAD).start()

        h_load(i).wait()
        qk = jnp.dot(h_v[i], wqk_v[...], preferred_element_type=jnp.float32).astype(jnp.bfloat16)
        q, k = qk[:, :cols], qk[:, cols:]
        q_s[i] = q
        k_s[i] = k
        qf, kf = q.astype(jnp.float32), k.astype(jnp.float32)
        q_sq = jnp.sum(qf * qf, axis=1, keepdims=True)
        k_sq = jnp.sum(kf * kf, axis=1, keepdims=True)
        lane = lax.broadcasted_iota(jnp.int32, (HEAD_DIM, HEAD_DIM), 1)
        rows = []
        for g in range(groups):
            part = slice(g * HEAD_DIM, (g + 1) * HEAD_DIM)
            both = jnp.where(lane == 0, q_sq[part], k_sq[part])
            rows.append(both.T[:2])
        stats[me, i] = jnp.concatenate(rows, axis=0)
        return carry

    lax.fori_loop(0, half, qk_block, 0)
    for load in tab_loads:
        load.start()
    send_stats(0)
    gather.send((1,))
    lax.fori_loop(half, n, qk_block, 0)
    send_stats(1)
    gather.send((2, 3))
    w_loads[2].wait()

    def v_block(i, carry):
        v = jnp.dot(h_v[i], wv_v[...], preferred_element_type=jnp.float32).astype(jnp.bfloat16)
        v_st[i] = lay(v)
        kv_store(1, i).start()
        vt_s[i] = v.T
        return carry

    lax.fori_loop(0, n, v_block, 0)
    for load in tab_loads:
        load.wait()

    def norm_block(j, carry):
        total = stats[0, j]
        for src in range(1, n):
            total = total + stats[src, j]
        inv = lax.rsqrt(total / width + EPS)
        inv_cols = jnp.concatenate([inv] * (HEAD_DIM // inv.shape[0]), axis=0).T
        for g in range(groups):
            part = slice(g * HEAD_DIM, (g + 1) * HEAD_DIM)
            tab = pl.ds(pl.multiple_of(j * tile + g * HEAD_DIM, HEAD_DIM), HEAD_DIM)
            cos, sin = cos_v[tab, :], sin_v[tab, :]
            for x_s, g_ref, col in ((q_s, qg_ref, 2 * g), (k_s, kg_ref, 2 * g + 1)):
                x = x_s[j, part, :].astype(jnp.float32) * inv_cols[:, col:col + 1] * g_ref[...]
                outs = []
                for hd in range(heads):
                    xh = x[:, hcols(hd)]
                    outs.append((xh * cos + pltpu.roll(xh, HEAD_DIM // 2, 1) * sin).astype(jnp.bfloat16))
                rot = jnp.concatenate(outs, axis=1)
                x_s[j, part, :] = rot
                if x_s is k_s:
                    k_st[j, part] = lay(rot)
        kv_store(0, j).start()
        return carry

    wait_stats(0)
    lax.fori_loop(0, half, norm_block, 0)
    wait_stats(1)
    lax.fori_loop(half, n, norm_block, 0)

    def o_copy(d):
        return pltpu.make_async_remote_copy(
            src_ref=o_s.at[d], dst_ref=o_hbm.at[:, pl.ds(pl.multiple_of(me * cols, cols), cols)],
            send_sem=o_send.at[d], recv_sem=o_recv.at[me], device_id=peer(d), device_id_type=MESH)

    def o_own():
        return pltpu.make_async_copy(o_s.at[0], o_hbm.at[:, pl.ds(pl.multiple_of(me * cols, cols), cols)], o_local)

    nt = (((1,), (1,)), ((), ()))
    strip = 64

    span = tile // SPLIT
    chains = [(hd, part) for hd in range(heads) for part in range(SPLIT)]

    def softmax_step(j, chain, m, l):
        hd, part = chain
        qs = slice(part * span, (part + 1) * span)
        top = None
        for c in range(tile // strip):
            best = jnp.max(s_buf[hd, c * strip:(c + 1) * strip, qs].reshape(strip // 8, 8, span), axis=0)
            top = best if top is None else jnp.maximum(top, best)
        m_new = jnp.max(top, axis=0, keepdims=True)
        if m is not None:
            m_new = jnp.maximum(m, m_new)
        m_scaled = m_new * scale
        total = None
        for c in range(tile // strip):
            p = jnp.exp2(s_buf[hd, c * strip:(c + 1) * strip, qs] * scale - m_scaled)
            add = jnp.sum(p.reshape(strip // 8, 8, span), axis=0)
            total = add if total is None else total + add
            p_buf[hd, c * strip:(c + 1) * strip, qs] = p.astype(jnp.bfloat16)
        l_new = jnp.sum(total, axis=0, keepdims=True)
        pv = jnp.dot(vt_s[j, hcols(hd), :], p_buf[hd, :, qs], preferred_element_type=jnp.float32)
        if m is None:
            acc_buf[hd, :, qs] = pv
        else:
            alpha = jnp.exp2((m - m_new) * scale)
            l_new = l * alpha + l_new
            acc_buf[hd, :, qs] = acc_buf[hd, :, qs] * alpha + pv
        return m_new, l_new

    def attend(step, carry):
        @pl.when(step == half)
        def _():
            gather.take((3, 7))

        d = lax.rem(step + 1, n)
        blk = lax.rem(me + d, n)

        def scores(j, chain):
            hd, part = chain
            return lax.dot_general(k_s[j, :, hcols(hd)], q_s[blk, part * span:(part + 1) * span, hcols(hd)], nt,
                                   preferred_element_type=jnp.float32)

        for hd, part in chains:
            keep = (lax.broadcasted_iota(jnp.int32, (tile, span), 0)
                    <= lax.broadcasted_iota(jnp.int32, (tile, span), 1) + part * span)
            s_buf[hd, :, part * span:(part + 1) * span] = jnp.where(keep, scores(blk, (hd, part)), -jnp.inf)
        state = tuple(softmax_step(blk, chain, None, None) for chain in chains)

        def body(j, state):
            for hd, part in chains:
                s_buf[hd, :, part * span:(part + 1) * span] = scores(j, (hd, part))
            return tuple(softmax_step(j, chain, *state[c]) for c, chain in enumerate(chains))

        state = lax.fori_loop(0, blk, body, state)
        for c, (hd, part) in enumerate(chains):
            qs = slice(part * span, (part + 1) * span)
            o_s[d, qs, hcols(hd)] = (acc_buf[hd, :, qs] / state[c][1]).T.astype(jnp.bfloat16)

        @pl.when(d != 0)
        def _():
            o_copy(d).start()

        @pl.when(d == 0)
        def _():
            o_own().start()
        return carry

    gather.relay()
    lax.fori_loop(0, n, attend, 0)
    gather.finish()
    o_own().wait()
    for d in range(1, n):
        src = lax.rem(me + d, n)
        o_copy(d).wait_send()
        pltpu.make_async_remote_copy(
            src_ref=o_s.at[d], dst_ref=o_hbm.at[:, pl.ds(pl.multiple_of(src * cols, cols), cols)],
            send_sem=o_send.at[d], recv_sem=o_recv.at[src], device_id=peer(d), device_id_type=MESH).wait_recv()
        for chunk in range(2):
            stats_copy(chunk, d).wait_send()
    for i in range(n):
        for which in range(2):
            kv_store(which, i).wait()


def block_call(n, h_full, wq, wk, wv, qg, kg, cos, sin, next_buf, cached):
    seq, width = h_full.shape
    cols = wq.shape[1]
    tile = seq // n
    heads = cols // HEAD_DIM
    next_rows = next_buf.shape[0] // n
    cache_tail = (heads, HEAD_DIM) if cached else (cols,)
    hbm = pl.BlockSpec(memory_space=pl.ANY)
    vmem = pl.BlockSpec(memory_space=pltpu.VMEM)
    flops = 2 * seq * width * cols * 3 + 2 * seq * seq * cols * 2
    cache = jax.ShapeDtypeStruct((seq,) + cache_tail, jnp.bfloat16)
    return pl.pallas_call(
        functools.partial(block_kernel, n, width),
        in_specs=[hbm, hbm, hbm, hbm, vmem, vmem, hbm, hbm, hbm],
        out_specs=[hbm, hbm, hbm, hbm],
        out_shape=[
            jax.ShapeDtypeStruct((tile, n * cols), jnp.bfloat16),
            jax.ShapeDtypeStruct(next_buf.shape, next_buf.dtype),
            cache, cache,
        ],
        input_output_aliases={8: 1},
        scratch_shapes=[
            pltpu.VMEM((n, tile, width), jnp.bfloat16),
            pltpu.VMEM((width, 2 * cols), jnp.bfloat16),
            pltpu.VMEM((width, cols), jnp.bfloat16),
            pltpu.VMEM((seq, HEAD_DIM), jnp.float32),
            pltpu.VMEM((seq, HEAD_DIM), jnp.float32),
            pltpu.VMEM((n, tile, cols), jnp.bfloat16),
            pltpu.VMEM((n, tile, cols), jnp.bfloat16),
            pltpu.VMEM((n, cols, tile), jnp.bfloat16),
            pltpu.VMEM((n, tile) + cache_tail, jnp.bfloat16),
            pltpu.VMEM((n, tile) + cache_tail, jnp.bfloat16),
            pltpu.VMEM((n, n, 2 * tile // HEAD_DIM, HEAD_DIM), jnp.float32),
            pltpu.VMEM((n, tile, cols), jnp.bfloat16),
            pltpu.VMEM((heads, tile, tile), jnp.float32),
            pltpu.VMEM((heads, tile, tile), jnp.bfloat16),
            pltpu.VMEM((heads, HEAD_DIM, tile), jnp.float32),
            pltpu.VMEM((3, next_rows, width), jnp.bfloat16),
            pltpu.SemaphoreType.DMA((n,)),
            pltpu.SemaphoreType.DMA((3,)),
            pltpu.SemaphoreType.DMA((2,)),
            pltpu.SemaphoreType.DMA((2, n)),
            pltpu.SemaphoreType.DMA((n, 2)),
            pltpu.SemaphoreType.DMA((n, 2)),
            pltpu.SemaphoreType.DMA((n,)),
            pltpu.SemaphoreType.DMA((n,)),
            pltpu.SemaphoreType.DMA,
        ] + GATHER_SEMS,
        compiler_params=pltpu.CompilerParams(
            collective_id=1 if cached else 2, has_side_effects=True, vmem_limit_bytes=62 * 1024 * 1024),
        cost_estimate=pl.CostEstimate(flops=flops, bytes_accessed=seq * width * 2 + 6 * seq * cols * 2, transcendentals=seq * seq * heads // 2),
        name='attn_block' if cached else 'attn_last',
    )(h_full, wq, wk, wv, qg, kg, cos, sin, next_buf)


N_CHUNK = 4


def last_kernel(n_batch, *refs):
    x_ref, wo_hbm = refs[:2]
    o_hbm = refs[2:2 + n_batch]
    rest = refs[2 + n_batch:]
    caches = rest[:2 * (n_batch - 1)]
    k_last, v_last = rest[2 * (n_batch - 1):2 * n_batch]
    out_ref, k_cache, v_cache = rest[2 * n_batch:2 * n_batch + 3]
    w_v, o_v, c_v, l_v, w_sem, o_sem, ci_sem, co_sem, lo_sem = rest[2 * n_batch + 3:]
    step = pl.program_id(0)
    b, j = step // N_CHUNK, lax.rem(step, N_CHUNK)
    chunk = w_v.shape[2]
    rows = c_v.shape[1]
    per = caches[0].shape[0] // rows
    slots = c_v.shape[0]

    def w_copy(c):
        return pltpu.make_async_copy(wo_hbm.at[:, pl.ds(c * chunk, chunk)], w_v.at[c], w_sem.at[c])

    def o_copy(i):
        return pltpu.make_async_copy(o_hbm[i], o_v.at[i], o_sem.at[i])

    @pl.when(step == 0)
    def _():
        w_copy(0).start()
        o_copy(0).start()
        for c in range(1, N_CHUNK):
            w_copy(c).start()
        for i in range(1, n_batch):
            o_copy(i).start()

    for i in range(n_batch):
        @pl.when(step == i * N_CHUNK)
        def _(i=i):
            o_copy(i).wait()
    for c in range(N_CHUNK):
        @pl.when(step == c)
        def _(c=c):
            w_copy(c).wait()

    items = [(i, part) for i in range(len(caches)) for part in range(per)]

    def item_in(t):
        i, part = items[t]
        return pltpu.make_async_copy(caches[i].at[pl.ds(part * rows, rows)], c_v.at[t % slots], ci_sem.at[t % slots])

    def item_out(t):
        i, part = items[t]
        cache = k_cache if i % 2 == 0 else v_cache
        return pltpu.make_async_copy(c_v.at[t % slots], cache.at[i // 2, pl.ds(part * rows, rows)], co_sem.at[t % slots])

    for t in range(len(items) + slots):
        @pl.when(step == t)
        def _(t=t):
            if t >= slots:
                item_out(t - slots).wait()
            if t < len(items):
                item_in(t).start()
            if 1 <= t <= len(items):
                item_in(t - 1).wait()
                item_out(t - 1).start()

    last_rows = l_v.shape[2]

    def last_out(which, t):
        cache = (k_cache, v_cache)[which]
        return pltpu.make_async_copy(l_v.at[which, lax.rem(t, 2)],
                                     cache.at[n_batch - 1, pl.ds(pl.multiple_of(t * last_rows, last_rows), last_rows)],
                                     lo_sem.at[which, lax.rem(t, 2)])

    @pl.when(step >= 2)
    def _():
        for which in range(2):
            last_out(which, step - 2).wait()
    for which, src in enumerate((k_last, v_last)):
        l_v[which, lax.rem(step, 2)] = src[...].reshape(l_v.shape[2:])
        last_out(which, step).start()

    y = jnp.dot(o_v[b], w_v[j], preferred_element_type=jnp.float32).astype(jnp.bfloat16)
    out_ref[0] = (x_ref[0].astype(jnp.float32) + y.astype(jnp.float32)).astype(jnp.bfloat16)

    @pl.when(step == n_batch * N_CHUNK - 1)
    def _():
        for which in range(2):
            for back in (1, 0):
                last_out(which, step - back).wait()


def last_call(x_local, w_o, os, ks, vs):
    n_batch, rows, width = x_local.shape
    seq, heads, _ = ks[0].shape
    steps = n_batch * N_CHUNK
    hbm = pl.BlockSpec(memory_space=pl.ANY)
    block = pl.BlockSpec((1, rows, width // N_CHUNK), lambda i: (i // N_CHUNK, 0, lax.rem(i, N_CHUNK)))
    last = pl.BlockSpec((seq // steps, heads * HEAD_DIM), lambda i: (i, 0))
    caches = [c for pair in zip(ks[:-1], vs[:-1]) for c in pair]
    cache = jax.ShapeDtypeStruct((n_batch, seq, heads, HEAD_DIM), jnp.bfloat16)
    return pl.pallas_call(
        functools.partial(last_kernel, n_batch),
        grid=(steps,),
        in_specs=[block, hbm] + [hbm] * (n_batch + len(caches)) + [last, last],
        out_specs=[block, hbm, hbm],
        out_shape=[jax.ShapeDtypeStruct(x_local.shape, jnp.bfloat16), cache, cache],
        scratch_shapes=[
            pltpu.VMEM((N_CHUNK, w_o.shape[0], width // N_CHUNK), jnp.bfloat16),
            pltpu.VMEM((n_batch, rows, w_o.shape[0]), jnp.bfloat16),
            pltpu.VMEM((4, 2048, heads, HEAD_DIM), jnp.bfloat16),
            pltpu.VMEM((2, 2, seq // steps, heads, HEAD_DIM), jnp.bfloat16),
            pltpu.SemaphoreType.DMA((N_CHUNK,)),
            pltpu.SemaphoreType.DMA((n_batch,)),
            pltpu.SemaphoreType.DMA((4,)),
            pltpu.SemaphoreType.DMA((4,)),
            pltpu.SemaphoreType.DMA((2, 2)),
        ],
        compiler_params=pltpu.CompilerParams(
            vmem_limit_bytes=52 * 1024 * 1024, dimension_semantics=('arbitrary',)),
        cost_estimate=pl.CostEstimate(flops=2 * n_batch * rows * width * w_o.shape[0],
                                      bytes_accessed=8 * n_batch * rows * width * 2, transcendentals=0),
        name='last_proj',
    )(x_local, w_o, *os, *caches, ks[-1], vs[-1])


def solution(mesh):
    n = mesh.shape['tp']
    assert n == 8 and tuple(mesh.axis_names) == ('dp', 'tp')

    def local_block(x_local, attn_gain, wq, wk, wv, qg, kg, wo_rows):
        n_batch, rows, width = x_local.shape
        cols = wq.shape[1]
        qg2, kg2 = qg.reshape(1, cols), kg.reshape(1, cols)
        half_dim = HEAD_DIM // 2
        inv_freq = 10000.0 ** (-jnp.arange(half_dim, dtype=jnp.float32) * (2.0 / HEAD_DIM))
        freq = jnp.concatenate([inv_freq, inv_freq]).reshape(1, HEAD_DIM)
        *hs, w_o, cos, sin = first_call(n, x_local, attn_gain.reshape(1, width), wo_rows, freq)
        os, ks, vs = [], [], []
        for b in range(n_batch):
            more = b + 1 < n_batch
            o, gathered, k, v = block_call(n, hs[b], wq, wk, wv, qg2, kg2, cos, sin, hs[b + 1] if more else w_o, more)
            if more:
                hs[b + 1] = gathered
            else:
                w_o = gathered
            os.append(o)
            ks.append(k)
            vs.append(v)
        return tuple(last_call(x_local, w_o, os, ks, vs))

    seq_spec = P('dp', 'tp', None)
    head_spec = P('dp', None, 'tp', None)
    col_spec = P(None, 'tp')
    return jax.shard_map(local_block, mesh=mesh, in_specs=(seq_spec, P(None), col_spec, col_spec, col_spec, P('tp'), P('tp'), P('tp', None)), out_specs=(seq_spec, head_spec, head_spec), check_vma=False)
```

```python
import functools
import math

import jax
import jax.numpy as jnp
from jax import lax
from jax.experimental import pallas as pl
from jax.experimental.pallas import tpu as pltpu
from jax.sharding import PartitionSpec as P

HEAD_DIM = 128
EPS = 1e-5
MESH = pl.DeviceIdType.MESH


FIRST = ((0, 2), (2, 1), (3, 1), (4, 4))
SECOND = ((4, 2), (6, 1), (7, 1), (0, 4))
PIECES = FIRST + SECOND + ((4, 2), (6, 2), (0, 2), (2, 2))
LAST = len(PIECES)


class RingGather:
    def __init__(self, buf, own, stage, me, ici_send, ici_recv, d2d_send, d2d_recv, keep):
        self.buf, self.own, self.stage, self.me, self.rows = buf, own, stage, me, stage.shape[1]
        self.ici_send, self.ici_recv, self.d2d_send, self.d2d_recv, self.keep = ici_send, ici_recv, d2d_send, d2d_recv, keep
        self.xn = me + 2 - 4 * lax.rem(me // 2, 2)
        self.yn = me + 4 - 8 * (me // 4)
        self.dg = self.yn + 2 - 4 * lax.rem(me // 2, 2)
        self.pt = me + 1 - 2 * lax.rem(me, 2)

    def block(self, block):
        return self.buf.at[pl.ds(pl.multiple_of(block * self.rows, self.rows), self.rows)]

    def span(self, piece):
        unit = self.rows // 8
        return PIECES[piece][0] * unit, PIECES[piece][1] * unit

    def slot(self, block, piece):
        first, rows = self.span(piece)
        unit = self.rows // 8
        return self.buf.at[pl.ds(pl.multiple_of(block * self.rows + first, unit), rows)]

    def staged(self, piece):
        first, rows = self.span(piece)
        which = 0 if piece < 4 else 1 if piece < 8 else 2
        return self.stage.at[which, pl.ds(first, rows)]

    def source(self, piece):
        return self.xn if piece < 4 else self.yn if piece < 8 else self.dg

    def copy(self, piece):
        first, rows = self.span(piece)
        if piece < 8:
            src = self.slot(self.me, piece) if self.own is None else self.own.at[pl.ds(first, rows)]
        else:
            src = self.stage.at[1 if piece < 10 else 0, pl.ds(first, rows)]
        return pltpu.make_async_remote_copy(
            src_ref=src, dst_ref=self.staged(piece), send_sem=self.ici_send.at[piece], recv_sem=self.ici_recv.at[piece],
            device_id={'tp': self.xn if piece < 4 or piece in (8, 9) else self.yn}, device_id_type=MESH)

    def handover(self, piece):
        if piece == LAST:
            dst = self.block(self.me)
            src = dst if self.own is None else self.own
        else:
            src, dst = self.staged(piece), self.slot(self.source(piece), piece)
        return pltpu.make_async_remote_copy(
            src_ref=src, dst_ref=dst, send_sem=self.d2d_send.at[piece], recv_sem=self.d2d_recv.at[piece],
            device_id={'tp': self.pt}, device_id_type=MESH)

    def store(self, piece):
        return pltpu.make_async_copy(self.staged(piece), self.slot(self.source(piece), piece), self.keep.at[piece])

    def send(self, turns):
        for turn in turns:
            self.copy(turn).start()
            self.copy(4 + turn).start()
        if 3 in turns:
            self.handover(LAST).start()

    def relay(self):
        for turns, onward in (((0,), 10), ((4,), 8), ((1, 2), 11), ((5, 6), 9)):
            for piece in turns:
                self.copy(piece).wait_recv()
            self.copy(onward).start()
        self.pass_on((0, 1, 2, 4, 5, 6))

    def pass_on(self, pieces):
        for piece in pieces:
            self.handover(piece).start()
            self.store(piece).start()

    def take(self, pieces):
        for piece in pieces:
            self.copy(piece).wait_recv()
            self.pass_on((piece,))

    def finish(self):
        self.take((8, 10, 9, 11))
        for piece in range(LAST):
            self.copy(piece).wait_send()
            self.store(piece).wait()
        for piece in range(LAST + 1):
            src = self.pt if piece == LAST else self.pt + self.source(piece) - self.me
            part = self.block(src) if piece == LAST else self.slot(src, piece)
            pltpu.make_async_remote_copy(
                src_ref=part, dst_ref=part, send_sem=self.d2d_send.at[piece], recv_sem=self.d2d_recv.at[piece],
                device_id={'tp': self.pt}, device_id_type=MESH).wait_recv()
            self.handover(piece).wait_send()


GATHER_SEMS = [pltpu.SemaphoreType.DMA((LAST,)), pltpu.SemaphoreType.DMA((LAST,)),
               pltpu.SemaphoreType.DMA((LAST + 1,)), pltpu.SemaphoreType.DMA((LAST + 1,)), pltpu.SemaphoreType.DMA((LAST,))]


def greet(n, me):
    barrier = pltpu.get_barrier_semaphore()
    for d in range(1, n):
        pl.semaphore_signal(barrier, inc=1, device_id={'tp': lax.rem(me + d, n)}, device_id_type=MESH)


def first_kernel(n, n_batch, x_hbm, gain_ref, wo_hbm, freq_ref,
                 h0, h1, h2, h3, wo_full, cos_hbm, sin_hbm,
                 x_v, h_v, wo_v, stage, cos_v, sin_v, in_sem, first_sem, wo_sem, out_sem, tab_sem, *gather_sems):
    me = lax.axis_index('tp')
    rows, width = x_v.shape[1:]
    wo_rows = wo_v.shape[0]
    hs = (h0, h1, h2, h3)
    greet(n, me)
    loads = [pltpu.make_async_copy(x_hbm.at[b], x_v.at[b], in_sem.at[b]) for b in range(1, n_batch)]
    wo_load = pltpu.make_async_copy(wo_hbm, wo_v, wo_sem.at[0])
    wo_store = pltpu.make_async_copy(wo_v, wo_full.at[pl.ds(pl.multiple_of(me * wo_rows, wo_rows), wo_rows)], wo_sem.at[1])
    stores = [pltpu.make_async_copy(h_v.at[b], hs[b].at[pl.ds(pl.multiple_of(me * rows, rows), rows)], out_sem.at[b])
              for b in range(n_batch)]
    fourth = rows // 4
    first_loads = [pltpu.make_async_copy(x_hbm.at[0, pl.ds(q * fourth, fourth)], x_v.at[0, pl.ds(q * fourth, fourth)],
                                         first_sem.at[q]) for q in range(4)]
    for q in (0, 2, 1, 3):
        first_loads[q].start()

    def norm(b, first=0, strips=rows // 64):
        def body(r, carry):
            part = pl.ds(pl.multiple_of(r * 64, 64), 64)
            x = x_v[b, part, :].astype(jnp.float32)
            inv = lax.rsqrt(jnp.mean(x * x, axis=-1, keepdims=True) + EPS)
            h_v[b, part, :] = (x * inv * gain_ref[...]).astype(jnp.bfloat16)
            return carry
        lax.fori_loop(first, first + strips, body, 0)

    quarter = rows // 256

    def norm_first(q):
        first_loads[q].wait()
        norm(0, q * quarter, quarter)

    norm_first(0)
    norm_first(2)
    pl.semaphore_wait(pltpu.get_barrier_semaphore(), n - 1)
    gather = RingGather(h0, h_v.at[0], stage, me, *gather_sems)
    gather.send((0,))
    norm_first(1)
    norm_first(3)
    gather.send((1, 2, 3))
    for load in loads:
        load.start()
    wo_load.start()
    stores[0].start()
    for b in range(1, n_batch):
        loads[b - 1].wait()
        norm(b)
        stores[b].start()
    wo_load.wait()
    wo_store.start()
    seq = cos_v.shape[0]

    def table(r, carry):
        part = pl.ds(pl.multiple_of(r * 64, 64), 64)
        pos = (lax.broadcasted_iota(jnp.int32, (64, HEAD_DIM), 0) + r * 64).astype(jnp.float32)
        lane = lax.broadcasted_iota(jnp.int32, (64, HEAD_DIM), 1)
        angle = pos * freq_ref[...]
        sin = jnp.sin(angle)
        cos_v[part, :] = jnp.cos(angle)
        sin_v[part, :] = jnp.where(lane < HEAD_DIM // 2, -sin, sin)
        return carry

    lax.fori_loop(0, seq // 64, table, 0)
    tables = [pltpu.make_async_copy(cos_v, cos_hbm, tab_sem.at[0]), pltpu.make_async_copy(sin_v, sin_hbm, tab_sem.at[1])]
    for copy in tables:
        copy.start()
    gather.relay()
    gather.take((3, 7))
    for copy in stores + [wo_store] + tables:
        copy.wait()
    gather.finish()


def first_call(n, x_local, gain, wo_rows, freq):
    n_batch, rows, width = x_local.shape
    depth = wo_rows.shape[0]
    seq = n * rows
    hbm = pl.BlockSpec(memory_space=pl.ANY)
    vmem = pl.BlockSpec(memory_space=pltpu.VMEM)
    return pl.pallas_call(
        functools.partial(first_kernel, n, n_batch),
        in_specs=[hbm, vmem, hbm, vmem],
        out_specs=[hbm] * (n_batch + 3),
        out_shape=[jax.ShapeDtypeStruct((seq, width), jnp.bfloat16)] * n_batch
        + [jax.ShapeDtypeStruct((n * depth, width), jnp.bfloat16)]
        + [jax.ShapeDtypeStruct((seq, HEAD_DIM), jnp.float32)] * 2,
        scratch_shapes=[
            pltpu.VMEM((n_batch, rows, width), jnp.bfloat16),
            pltpu.VMEM((n_batch, rows, width), jnp.bfloat16),
            pltpu.VMEM((depth, width), jnp.bfloat16),
            pltpu.VMEM((3, rows, width), jnp.bfloat16),
            pltpu.VMEM((seq, HEAD_DIM), jnp.float32),
            pltpu.VMEM((seq, HEAD_DIM), jnp.float32),
            pltpu.SemaphoreType.DMA((n_batch,)),
            pltpu.SemaphoreType.DMA((4,)),
            pltpu.SemaphoreType.DMA((2,)),
            pltpu.SemaphoreType.DMA((n_batch,)),
            pltpu.SemaphoreType.DMA((2,)),
        ] + GATHER_SEMS,
        compiler_params=pltpu.CompilerParams(
            collective_id=0, has_side_effects=True, vmem_limit_bytes=62 * 1024 * 1024),
        cost_estimate=pl.CostEstimate(flops=100000000, bytes_accessed=seq * width * 4, transcendentals=seq * HEAD_DIM * 2),
        name='first_gather',
    )(x_local, gain, wo_rows, freq)


AHEAD = 3
SPLIT = 2


def block_kernel(n, width, h_hbm, wq_hbm, wk_hbm, wv_hbm, qg_ref, kg_ref, cos_hbm, sin_hbm, next_in,
                 o_hbm, next_buf, k_out, v_out,
                 h_v, wqk_v, wv_v, cos_v, sin_v, q_s, k_s, vt_s, k_st, v_st, stats, o_s, s_buf, p_buf, acc_buf, stage,
                 h_sem, w_sem, tab_sem, kv_sem, st_send, st_recv, o_send, o_recv, o_local, *gather_sems):
    me = lax.axis_index('tp')
    tile = h_v.shape[1]
    cols = wv_v.shape[1]
    heads = cols // HEAD_DIM
    groups = tile // HEAD_DIM
    half = n // 2
    gather = RingGather(next_buf, None, stage, me, *gather_sems)
    scale = HEAD_DIM ** -0.5 * math.log2(math.e)

    def peer(d):
        return {'tp': lax.rem(me + d, n)}

    def stats_copy(chunk, d):
        part = stats.at[me, pl.ds(chunk * half, half)]
        return pltpu.make_async_remote_copy(
            src_ref=part, dst_ref=part, send_sem=st_send.at[d, chunk], recv_sem=st_recv.at[me, chunk],
            device_id=peer(d), device_id_type=MESH)

    def send_stats(chunk):
        for d in range(1, n):
            stats_copy(chunk, d).start()

    def wait_stats(chunk):
        for d in range(1, n):
            src = lax.rem(me + d, n)
            part = stats.at[src, pl.ds(chunk * half, half)]
            pltpu.make_async_remote_copy(
                src_ref=part, dst_ref=part, send_sem=st_send.at[d, chunk], recv_sem=st_recv.at[src, chunk],
                device_id=peer(d), device_id_type=MESH).wait_recv()

    def lay(x):
        return x if len(k_out.shape) == 2 else x.reshape(x.shape[0], heads, HEAD_DIM)

    def hcols(hd):
        return slice(hd * HEAD_DIM, (hd + 1) * HEAD_DIM)

    def rows_of(i):
        return pl.ds(pl.multiple_of(i * tile, tile), tile)

    def h_load(i):
        return pltpu.make_async_copy(h_hbm.at[rows_of(i)], h_v.at[i], h_sem.at[i])

    def kv_store(which, i):
        src, dst = ((k_st, k_out), (v_st, v_out))[which]
        return pltpu.make_async_copy(src.at[i], dst.at[rows_of(i)], kv_sem.at[which, i])

    w_loads = [
        pltpu.make_async_copy(wq_hbm, wqk_v.at[:, pl.ds(0, cols)], w_sem.at[0]),
        pltpu.make_async_copy(wk_hbm, wqk_v.at[:, pl.ds(cols, cols)], w_sem.at[1]),
        pltpu.make_async_copy(wv_hbm, wv_v, w_sem.at[2])]
    tab_loads = [pltpu.make_async_copy(cos_hbm, cos_v, tab_sem.at[0]), pltpu.make_async_copy(sin_hbm, sin_v, tab_sem.at[1])]

    greet(n, me)
    for load in w_loads[:2] + [h_load(i) for i in range(AHEAD)] + w_loads[2:]:
        load.start()
    pl.semaphore_wait(pltpu.get_barrier_semaphore(), n - 1)
    gather.send((0,))
    for load in w_loads[:2]:
        load.wait()

    def qk_block(i, carry):
        @pl.when(i + AHEAD < n)
        def _():
            h_load(i + AHEAD).start()

        h_load(i).wait()
        qk = jnp.dot(h_v[i], wqk_v[...], preferred_element_type=jnp.float32).astype(jnp.bfloat16)
        q, k = qk[:, :cols], qk[:, cols:]
        q_s[i] = q
        k_s[i] = k
        qf, kf = q.astype(jnp.float32), k.astype(jnp.float32)
        q_sq = jnp.sum(qf * qf, axis=1, keepdims=True)
        k_sq = jnp.sum(kf * kf, axis=1, keepdims=True)
        lane = lax.broadcasted_iota(jnp.int32, (HEAD_DIM, HEAD_DIM), 1)
        rows = []
        for g in range(groups):
            part = slice(g * HEAD_DIM, (g + 1) * HEAD_DIM)
            both = jnp.where(lane == 0, q_sq[part], k_sq[part])
            rows.append(both.T[:2])
        stats[me, i] = jnp.concatenate(rows, axis=0)
        return carry

    lax.fori_loop(0, half, qk_block, 0)
    for load in tab_loads:
        load.start()
    send_stats(0)
    gather.send((1,))
    lax.fori_loop(half, n, qk_block, 0)
    send_stats(1)
    gather.send((2, 3))
    w_loads[2].wait()

    def v_block(i, carry):
        v = jnp.dot(h_v[i], wv_v[...], preferred_element_type=jnp.float32).astype(jnp.bfloat16)
        v_st[i] = lay(v)
        kv_store(1, i).start()
        vt_s[i] = v.T
        return carry

    lax.fori_loop(0, n, v_block, 0)
    for load in tab_loads:
        load.wait()

    def norm_block(j, carry):
        total = stats[0, j]
        for src in range(1, n):
            total = total + stats[src, j]
        inv = lax.rsqrt(total / width + EPS)
        inv_cols = jnp.concatenate([inv] * (HEAD_DIM // inv.shape[0]), axis=0).T
        for g in range(groups):
            part = slice(g * HEAD_DIM, (g + 1) * HEAD_DIM)
            tab = pl.ds(pl.multiple_of(j * tile + g * HEAD_DIM, HEAD_DIM), HEAD_DIM)
            cos, sin = cos_v[tab, :], sin_v[tab, :]
            for x_s, g_ref, col in ((q_s, qg_ref, 2 * g), (k_s, kg_ref, 2 * g + 1)):
                x = x_s[j, part, :].astype(jnp.float32) * inv_cols[:, col:col + 1] * g_ref[...]
                outs = []
                for hd in range(heads):
                    xh = x[:, hcols(hd)]
                    outs.append((xh * cos + pltpu.roll(xh, HEAD_DIM // 2, 1) * sin).astype(jnp.bfloat16))
                rot = jnp.concatenate(outs, axis=1)
                x_s[j, part, :] = rot
                if x_s is k_s:
                    k_st[j, part] = lay(rot)
        kv_store(0, j).start()
        return carry

    wait_stats(0)
    lax.fori_loop(0, half, norm_block, 0)
    wait_stats(1)
    lax.fori_loop(half, n, norm_block, 0)

    def o_copy(d):
        return pltpu.make_async_remote_copy(
            src_ref=o_s.at[d], dst_ref=o_hbm.at[:, pl.ds(pl.multiple_of(me * cols, cols), cols)],
            send_sem=o_send.at[d], recv_sem=o_recv.at[me], device_id=peer(d), device_id_type=MESH)

    def o_own():
        return pltpu.make_async_copy(o_s.at[0], o_hbm.at[:, pl.ds(pl.multiple_of(me * cols, cols), cols)], o_local)

    nt = (((1,), (1,)), ((), ()))
    strip = 64

    span = tile // SPLIT
    chains = [(hd, part) for hd in range(heads) for part in range(SPLIT)]

    def softmax_step(j, chain, m, l, keys):
        hd, part = chain
        qs = slice(part * span, (part + 1) * span)
        top = None
        for c in range(keys // strip):
            best = jnp.max(s_buf[hd, c * strip:(c + 1) * strip, qs].reshape(strip // 8, 8, span), axis=0)
            top = best if top is None else jnp.maximum(top, best)
        m_new = jnp.max(top, axis=0, keepdims=True)
        if m is not None:
            m_new = jnp.maximum(m, m_new)
        m_scaled = m_new * scale
        total = None
        for c in range(keys // strip):
            p = jnp.exp2(s_buf[hd, c * strip:(c + 1) * strip, qs] * scale - m_scaled)
            add = jnp.sum(p.reshape(strip // 8, 8, span), axis=0)
            total = add if total is None else total + add
            p_buf[hd, c * strip:(c + 1) * strip, qs] = p.astype(jnp.bfloat16)
        l_new = jnp.sum(total, axis=0, keepdims=True)
        pv = jnp.dot(vt_s[j, hcols(hd), :keys], p_buf[hd, :keys, qs], preferred_element_type=jnp.float32)
        if m is None:
            acc_buf[hd, :, qs] = pv
        else:
            alpha = jnp.exp2((m - m_new) * scale)
            l_new = l * alpha + l_new
            acc_buf[hd, :, qs] = acc_buf[hd, :, qs] * alpha + pv
        return m_new, l_new

    def attend(step, carry):
        @pl.when(step == half)
        def _():
            gather.take((3, 7))

        d = lax.rem(step + 1, n)
        blk = lax.rem(me + d, n)

        def scores(j, chain, keys=tile):
            hd, part = chain
            return lax.dot_general(k_s[j, :keys, hcols(hd)], q_s[blk, part * span:(part + 1) * span, hcols(hd)], nt,
                                   preferred_element_type=jnp.float32)

        for hd, part in chains:
            keys = (part + 1) * span
            keep = (lax.broadcasted_iota(jnp.int32, (keys, span), 0)
                    <= lax.broadcasted_iota(jnp.int32, (keys, span), 1) + part * span)
            s_buf[hd, :keys, part * span:keys] = jnp.where(keep, scores(blk, (hd, part), keys), -jnp.inf)
        state = tuple(softmax_step(blk, chain, None, None, (chain[1] + 1) * span) for chain in chains)

        def body(j, state):
            for hd, part in chains:
                s_buf[hd, :, part * span:(part + 1) * span] = scores(j, (hd, part))
            return tuple(softmax_step(j, chain, *state[c], tile) for c, chain in enumerate(chains))

        state = lax.fori_loop(0, blk, body, state)
        for c, (hd, part) in enumerate(chains):
            qs = slice(part * span, (part + 1) * span)
            o_s[d, qs, hcols(hd)] = (acc_buf[hd, :, qs] / state[c][1]).T.astype(jnp.bfloat16)

        @pl.when(d != 0)
        def _():
            o_copy(d).start()

        @pl.when(d == 0)
        def _():
            o_own().start()
        return carry

    gather.relay()
    lax.fori_loop(0, n, attend, 0)
    gather.finish()
    o_own().wait()
    for d in range(1, n):
        src = lax.rem(me + d, n)
        o_copy(d).wait_send()
        pltpu.make_async_remote_copy(
            src_ref=o_s.at[d], dst_ref=o_hbm.at[:, pl.ds(pl.multiple_of(src * cols, cols), cols)],
            send_sem=o_send.at[d], recv_sem=o_recv.at[src], device_id=peer(d), device_id_type=MESH).wait_recv()
        for chunk in range(2):
            stats_copy(chunk, d).wait_send()
    for i in range(n):
        for which in range(2):
            kv_store(which, i).wait()


def block_call(n, h_full, wq, wk, wv, qg, kg, cos, sin, next_buf, cached):
    seq, width = h_full.shape
    cols = wq.shape[1]
    tile = seq // n
    heads = cols // HEAD_DIM
    next_rows = next_buf.shape[0] // n
    cache_tail = (heads, HEAD_DIM) if cached else (cols,)
    hbm = pl.BlockSpec(memory_space=pl.ANY)
    vmem = pl.BlockSpec(memory_space=pltpu.VMEM)
    flops = 2 * seq * width * cols * 3 + 2 * seq * seq * cols * 2
    cache = jax.ShapeDtypeStruct((seq,) + cache_tail, jnp.bfloat16)
    return pl.pallas_call(
        functools.partial(block_kernel, n, width),
        in_specs=[hbm, hbm, hbm, hbm, vmem, vmem, hbm, hbm, hbm],
        out_specs=[hbm, hbm, hbm, hbm],
        out_shape=[
            jax.ShapeDtypeStruct((tile, n * cols), jnp.bfloat16),
            jax.ShapeDtypeStruct(next_buf.shape, next_buf.dtype),
            cache, cache,
        ],
        input_output_aliases={8: 1},
        scratch_shapes=[
            pltpu.VMEM((n, tile, width), jnp.bfloat16),
            pltpu.VMEM((width, 2 * cols), jnp.bfloat16),
            pltpu.VMEM((width, cols), jnp.bfloat16),
            pltpu.VMEM((seq, HEAD_DIM), jnp.float32),
            pltpu.VMEM((seq, HEAD_DIM), jnp.float32),
            pltpu.VMEM((n, tile, cols), jnp.bfloat16),
            pltpu.VMEM((n, tile, cols), jnp.bfloat16),
            pltpu.VMEM((n, cols, tile), jnp.bfloat16),
            pltpu.VMEM((n, tile) + cache_tail, jnp.bfloat16),
            pltpu.VMEM((n, tile) + cache_tail, jnp.bfloat16),
            pltpu.VMEM((n, n, 2 * tile // HEAD_DIM, HEAD_DIM), jnp.float32),
            pltpu.VMEM((n, tile, cols), jnp.bfloat16),
            pltpu.VMEM((heads, tile, tile), jnp.float32),
            pltpu.VMEM((heads, tile, tile), jnp.bfloat16),
            pltpu.VMEM((heads, HEAD_DIM, tile), jnp.float32),
            pltpu.VMEM((3, next_rows, width), jnp.bfloat16),
            pltpu.SemaphoreType.DMA((n,)),
            pltpu.SemaphoreType.DMA((3,)),
            pltpu.SemaphoreType.DMA((2,)),
            pltpu.SemaphoreType.DMA((2, n)),
            pltpu.SemaphoreType.DMA((n, 2)),
            pltpu.SemaphoreType.DMA((n, 2)),
            pltpu.SemaphoreType.DMA((n,)),
            pltpu.SemaphoreType.DMA((n,)),
            pltpu.SemaphoreType.DMA,
        ] + GATHER_SEMS,
        compiler_params=pltpu.CompilerParams(
            collective_id=1 if cached else 2, has_side_effects=True, vmem_limit_bytes=62 * 1024 * 1024),
        cost_estimate=pl.CostEstimate(flops=flops, bytes_accessed=seq * width * 2 + 6 * seq * cols * 2, transcendentals=seq * seq * heads // 2),
        name='attn_block' if cached else 'attn_last',
    )(h_full, wq, wk, wv, qg, kg, cos, sin, next_buf)


N_CHUNK = 4


def last_kernel(n_batch, *refs):
    x_ref, wo_hbm = refs[:2]
    o_hbm = refs[2:2 + n_batch]
    rest = refs[2 + n_batch:]
    caches = rest[:2 * (n_batch - 1)]
    k_last, v_last = rest[2 * (n_batch - 1):2 * n_batch]
    out_ref, k_cache, v_cache = rest[2 * n_batch:2 * n_batch + 3]
    w_v, o_v, c_v, l_v, w_sem, o_sem, ci_sem, co_sem, lo_sem = rest[2 * n_batch + 3:]
    step = pl.program_id(0)
    b, j = step // N_CHUNK, lax.rem(step, N_CHUNK)
    chunk = w_v.shape[2]
    rows = c_v.shape[1]
    per = caches[0].shape[0] // rows
    slots = c_v.shape[0]

    def w_copy(c):
        return pltpu.make_async_copy(wo_hbm.at[:, pl.ds(c * chunk, chunk)], w_v.at[c], w_sem.at[c])

    def o_copy(i):
        return pltpu.make_async_copy(o_hbm[i], o_v.at[i], o_sem.at[i])

    @pl.when(step == 0)
    def _():
        w_copy(0).start()
        o_copy(0).start()
        for c in range(1, N_CHUNK):
            w_copy(c).start()
        for i in range(1, n_batch):
            o_copy(i).start()

    for i in range(n_batch):
        @pl.when(step == i * N_CHUNK)
        def _(i=i):
            o_copy(i).wait()
    for c in range(N_CHUNK):
        @pl.when(step == c)
        def _(c=c):
            w_copy(c).wait()

    items = [(i, part) for i in range(len(caches)) for part in range(per)]

    def item_in(t):
        i, part = items[t]
        return pltpu.make_async_copy(caches[i].at[pl.ds(part * rows, rows)], c_v.at[t % slots], ci_sem.at[t % slots])

    def item_out(t):
        i, part = items[t]
        cache = k_cache if i % 2 == 0 else v_cache
        return pltpu.make_async_copy(c_v.at[t % slots], cache.at[i // 2, pl.ds(part * rows, rows)], co_sem.at[t % slots])

    for t in range(len(items) + slots):
        @pl.when(step == t)
        def _(t=t):
            if t >= slots:
                item_out(t - slots).wait()
            if t < len(items):
                item_in(t).start()
            if 1 <= t <= len(items):
                item_in(t - 1).wait()
                item_out(t - 1).start()

    last_rows = l_v.shape[2]

    def last_out(which, t):
        cache = (k_cache, v_cache)[which]
        return pltpu.make_async_copy(l_v.at[which, lax.rem(t, 2)],
                                     cache.at[n_batch - 1, pl.ds(pl.multiple_of(t * last_rows, last_rows), last_rows)],
                                     lo_sem.at[which, lax.rem(t, 2)])

    @pl.when(step >= 2)
    def _():
        for which in range(2):
            last_out(which, step - 2).wait()
    for which, src in enumerate((k_last, v_last)):
        l_v[which, lax.rem(step, 2)] = src[...].reshape(l_v.shape[2:])
        last_out(which, step).start()

    y = jnp.dot(o_v[b], w_v[j], preferred_element_type=jnp.float32).astype(jnp.bfloat16)
    out_ref[0] = (x_ref[0].astype(jnp.float32) + y.astype(jnp.float32)).astype(jnp.bfloat16)

    @pl.when(step == n_batch * N_CHUNK - 1)
    def _():
        for which in range(2):
            for back in (1, 0):
                last_out(which, step - back).wait()


def last_call(x_local, w_o, os, ks, vs):
    n_batch, rows, width = x_local.shape
    seq, heads, _ = ks[0].shape
    steps = n_batch * N_CHUNK
    hbm = pl.BlockSpec(memory_space=pl.ANY)
    block = pl.BlockSpec((1, rows, width // N_CHUNK), lambda i: (i // N_CHUNK, 0, lax.rem(i, N_CHUNK)))
    last = pl.BlockSpec((seq // steps, heads * HEAD_DIM), lambda i: (i, 0))
    caches = [c for pair in zip(ks[:-1], vs[:-1]) for c in pair]
    cache = jax.ShapeDtypeStruct((n_batch, seq, heads, HEAD_DIM), jnp.bfloat16)
    return pl.pallas_call(
        functools.partial(last_kernel, n_batch),
        grid=(steps,),
        in_specs=[block, hbm] + [hbm] * (n_batch + len(caches)) + [last, last],
        out_specs=[block, hbm, hbm],
        out_shape=[jax.ShapeDtypeStruct(x_local.shape, jnp.bfloat16), cache, cache],
        scratch_shapes=[
            pltpu.VMEM((N_CHUNK, w_o.shape[0], width // N_CHUNK), jnp.bfloat16),
            pltpu.VMEM((n_batch, rows, w_o.shape[0]), jnp.bfloat16),
            pltpu.VMEM((4, 2048, heads, HEAD_DIM), jnp.bfloat16),
            pltpu.VMEM((2, 2, seq // steps, heads, HEAD_DIM), jnp.bfloat16),
            pltpu.SemaphoreType.DMA((N_CHUNK,)),
            pltpu.SemaphoreType.DMA((n_batch,)),
            pltpu.SemaphoreType.DMA((4,)),
            pltpu.SemaphoreType.DMA((4,)),
            pltpu.SemaphoreType.DMA((2, 2)),
        ],
        compiler_params=pltpu.CompilerParams(
            vmem_limit_bytes=52 * 1024 * 1024, dimension_semantics=('arbitrary',)),
        cost_estimate=pl.CostEstimate(flops=2 * n_batch * rows * width * w_o.shape[0],
                                      bytes_accessed=8 * n_batch * rows * width * 2, transcendentals=0),
        name='last_proj',
    )(x_local, w_o, *os, *caches, ks[-1], vs[-1])


def solution(mesh):
    n = mesh.shape['tp']
    assert n == 8 and tuple(mesh.axis_names) == ('dp', 'tp')

    def local_block(x_local, attn_gain, wq, wk, wv, qg, kg, wo_rows):
        n_batch, rows, width = x_local.shape
        cols = wq.shape[1]
        qg2, kg2 = qg.reshape(1, cols), kg.reshape(1, cols)
        half_dim = HEAD_DIM // 2
        inv_freq = 10000.0 ** (-jnp.arange(half_dim, dtype=jnp.float32) * (2.0 / HEAD_DIM))
        freq = jnp.concatenate([inv_freq, inv_freq]).reshape(1, HEAD_DIM)
        *hs, w_o, cos, sin = first_call(n, x_local, attn_gain.reshape(1, width), wo_rows, freq)
        os, ks, vs = [], [], []
        for b in range(n_batch):
            more = b + 1 < n_batch
            o, gathered, k, v = block_call(n, hs[b], wq, wk, wv, qg2, kg2, cos, sin, hs[b + 1] if more else w_o, more)
            if more:
                hs[b + 1] = gathered
            else:
                w_o = gathered
            os.append(o)
            ks.append(k)
            vs.append(v)
        return tuple(last_call(x_local, w_o, os, ks, vs))

    seq_spec = P('dp', 'tp', None)
    head_spec = P('dp', None, 'tp', None)
    col_spec = P(None, 'tp')
    return jax.shard_map(local_block, mesh=mesh, in_specs=(seq_spec, P(None), col_spec, col_spec, col_spec, P('tp'), P('tp'), P('tp', None)), out_specs=(seq_spec, head_spec, head_spec), check_vma=False)
```

```python
import functools
import math

import jax
import jax.numpy as jnp
from jax import lax
from jax.experimental import pallas as pl
from jax.experimental.pallas import tpu as pltpu
from jax.sharding import PartitionSpec as P

HEAD_DIM = 128
EPS = 1e-5
MESH = pl.DeviceIdType.MESH


FIRST = ((0, 2), (2, 1), (3, 1), (4, 4))
SECOND = ((4, 2), (6, 1), (7, 1), (0, 4))
PIECES = FIRST + SECOND + ((4, 2), (6, 2), (0, 2), (2, 2))
LAST = len(PIECES)


class RingGather:
    def __init__(self, buf, own, stage, me, ici_send, ici_recv, d2d_send, d2d_recv, keep):
        self.buf, self.own, self.stage, self.me, self.rows = buf, own, stage, me, stage.shape[1]
        self.ici_send, self.ici_recv, self.d2d_send, self.d2d_recv, self.keep = ici_send, ici_recv, d2d_send, d2d_recv, keep
        self.xn = me + 2 - 4 * lax.rem(me // 2, 2)
        self.yn = me + 4 - 8 * (me // 4)
        self.dg = self.yn + 2 - 4 * lax.rem(me // 2, 2)
        self.pt = me + 1 - 2 * lax.rem(me, 2)

    def block(self, block):
        return self.buf.at[pl.ds(pl.multiple_of(block * self.rows, self.rows), self.rows)]

    def span(self, piece):
        unit = self.rows // 8
        return PIECES[piece][0] * unit, PIECES[piece][1] * unit

    def slot(self, block, piece):
        first, rows = self.span(piece)
        unit = self.rows // 8
        return self.buf.at[pl.ds(pl.multiple_of(block * self.rows + first, unit), rows)]

    def staged(self, piece):
        first, rows = self.span(piece)
        which = 0 if piece < 4 else 1 if piece < 8 else 2
        return self.stage.at[which, pl.ds(first, rows)]

    def source(self, piece):
        return self.xn if piece < 4 else self.yn if piece < 8 else self.dg

    def copy(self, piece):
        first, rows = self.span(piece)
        if piece < 8:
            src = self.slot(self.me, piece) if self.own is None else self.own.at[pl.ds(first, rows)]
        else:
            src = self.stage.at[1 if piece < 10 else 0, pl.ds(first, rows)]
        return pltpu.make_async_remote_copy(
            src_ref=src, dst_ref=self.staged(piece), send_sem=self.ici_send.at[piece], recv_sem=self.ici_recv.at[piece],
            device_id={'tp': self.xn if piece < 4 or piece in (8, 9) else self.yn}, device_id_type=MESH)

    def handover(self, piece):
        if piece == LAST:
            dst = self.block(self.me)
            src = dst if self.own is None else self.own
        else:
            src, dst = self.staged(piece), self.slot(self.source(piece), piece)
        return pltpu.make_async_remote_copy(
            src_ref=src, dst_ref=dst, send_sem=self.d2d_send.at[piece], recv_sem=self.d2d_recv.at[piece],
            device_id={'tp': self.pt}, device_id_type=MESH)

    def store(self, piece):
        return pltpu.make_async_copy(self.staged(piece), self.slot(self.source(piece), piece), self.keep.at[piece])

    def send(self, turns):
        for turn in turns:
            self.copy(turn).start()
            self.copy(4 + turn).start()
        if 3 in turns:
            self.handover(LAST).start()

    def relay(self):
        for turns, onward in (((0,), 10), ((4,), 8), ((1, 2), 11), ((5, 6), 9)):
            for piece in turns:
                self.copy(piece).wait_recv()
            self.copy(onward).start()
        self.pass_on((0, 1, 2, 4, 5, 6))

    def pass_on(self, pieces):
        for piece in pieces:
            self.handover(piece).start()
            self.store(piece).start()

    def take(self, pieces):
        for piece in pieces:
            self.copy(piece).wait_recv()
            self.pass_on((piece,))

    def finish(self):
        self.take((8, 10, 9, 11))
        for piece in range(LAST):
            self.copy(piece).wait_send()
            self.store(piece).wait()
        for piece in range(LAST + 1):
            src = self.pt if piece == LAST else self.pt + self.source(piece) - self.me
            part = self.block(src) if piece == LAST else self.slot(src, piece)
            pltpu.make_async_remote_copy(
                src_ref=part, dst_ref=part, send_sem=self.d2d_send.at[piece], recv_sem=self.d2d_recv.at[piece],
                device_id={'tp': self.pt}, device_id_type=MESH).wait_recv()
            self.handover(piece).wait_send()


GATHER_SEMS = [pltpu.SemaphoreType.DMA((LAST,)), pltpu.SemaphoreType.DMA((LAST,)),
               pltpu.SemaphoreType.DMA((LAST + 1,)), pltpu.SemaphoreType.DMA((LAST + 1,)), pltpu.SemaphoreType.DMA((LAST,))]


def greet(n, me):
    barrier = pltpu.get_barrier_semaphore()
    for d in range(1, n):
        pl.semaphore_signal(barrier, inc=1, device_id={'tp': lax.rem(me + d, n)}, device_id_type=MESH)


def first_kernel(n, n_batch, x_hbm, gain_ref, wo_hbm, freq_ref,
                 h0, h1, h2, h3, wo_full, cos_hbm, sin_hbm,
                 x_v, h_v, wo_v, stage, cos_v, sin_v, in_sem, first_sem, wo_sem, out_sem, tab_sem, *gather_sems):
    me = lax.axis_index('tp')
    rows, width = x_v.shape[1:]
    wo_rows = wo_v.shape[0]
    hs = (h0, h1, h2, h3)
    greet(n, me)
    loads = [pltpu.make_async_copy(x_hbm.at[b], x_v.at[b], in_sem.at[b]) for b in range(1, n_batch)]
    wo_load = pltpu.make_async_copy(wo_hbm, wo_v, wo_sem.at[0])
    wo_store = pltpu.make_async_copy(wo_v, wo_full.at[pl.ds(pl.multiple_of(me * wo_rows, wo_rows), wo_rows)], wo_sem.at[1])
    stores = [pltpu.make_async_copy(h_v.at[b], hs[b].at[pl.ds(pl.multiple_of(me * rows, rows), rows)], out_sem.at[b])
              for b in range(n_batch)]
    fourth = rows // 4
    first_loads = [pltpu.make_async_copy(x_hbm.at[0, pl.ds(q * fourth, fourth)], x_v.at[0, pl.ds(q * fourth, fourth)],
                                         first_sem.at[q]) for q in range(4)]
    for q in (0, 2, 1, 3):
        first_loads[q].start()

    def norm(b, first=0, strips=rows // 64):
        def body(r, carry):
            part = pl.ds(pl.multiple_of(r * 64, 64), 64)
            x = x_v[b, part, :].astype(jnp.float32)
            inv = lax.rsqrt(jnp.mean(x * x, axis=-1, keepdims=True) + EPS)
            h_v[b, part, :] = (x * inv * gain_ref[...]).astype(jnp.bfloat16)
            return carry
        lax.fori_loop(first, first + strips, body, 0)

    quarter = rows // 256

    def norm_first(q):
        first_loads[q].wait()
        norm(0, q * quarter, quarter)

    norm_first(0)
    norm_first(2)
    pl.semaphore_wait(pltpu.get_barrier_semaphore(), n - 1)
    gather = RingGather(h0, h_v.at[0], stage, me, *gather_sems)
    gather.send((0,))
    norm_first(1)
    norm_first(3)
    gather.send((1, 2, 3))
    for load in loads:
        load.start()
    wo_load.start()
    stores[0].start()
    for b in range(1, n_batch):
        loads[b - 1].wait()
        norm(b)
        stores[b].start()
    wo_load.wait()
    wo_store.start()
    seq = cos_v.shape[0]

    def table(r, carry):
        part = pl.ds(pl.multiple_of(r * 64, 64), 64)
        pos = (lax.broadcasted_iota(jnp.int32, (64, HEAD_DIM), 0) + r * 64).astype(jnp.float32)
        lane = lax.broadcasted_iota(jnp.int32, (64, HEAD_DIM), 1)
        angle = pos * freq_ref[...]
        sin = jnp.sin(angle)
        cos_v[part, :] = jnp.cos(angle)
        sin_v[part, :] = jnp.where(lane < HEAD_DIM // 2, -sin, sin)
        return carry

    lax.fori_loop(0, seq // 64, table, 0)
    tables = [pltpu.make_async_copy(cos_v, cos_hbm, tab_sem.at[0]), pltpu.make_async_copy(sin_v, sin_hbm, tab_sem.at[1])]
    for copy in tables:
        copy.start()
    gather.relay()
    gather.take((3, 7))
    for copy in stores + [wo_store] + tables:
        copy.wait()
    gather.finish()


def first_call(n, x_local, gain, wo_rows, freq):
    n_batch, rows, width = x_local.shape
    depth = wo_rows.shape[0]
    seq = n * rows
    hbm = pl.BlockSpec(memory_space=pl.ANY)
    vmem = pl.BlockSpec(memory_space=pltpu.VMEM)
    return pl.pallas_call(
        functools.partial(first_kernel, n, n_batch),
        in_specs=[hbm, vmem, hbm, vmem],
        out_specs=[hbm] * (n_batch + 3),
        out_shape=[jax.ShapeDtypeStruct((seq, width), jnp.bfloat16)] * n_batch
        + [jax.ShapeDtypeStruct((n * depth, width), jnp.bfloat16)]
        + [jax.ShapeDtypeStruct((seq, HEAD_DIM), jnp.float32)] * 2,
        scratch_shapes=[
            pltpu.VMEM((n_batch, rows, width), jnp.bfloat16),
            pltpu.VMEM((n_batch, rows, width), jnp.bfloat16),
            pltpu.VMEM((depth, width), jnp.bfloat16),
            pltpu.VMEM((3, rows, width), jnp.bfloat16),
            pltpu.VMEM((seq, HEAD_DIM), jnp.float32),
            pltpu.VMEM((seq, HEAD_DIM), jnp.float32),
            pltpu.SemaphoreType.DMA((n_batch,)),
            pltpu.SemaphoreType.DMA((4,)),
            pltpu.SemaphoreType.DMA((2,)),
            pltpu.SemaphoreType.DMA((n_batch,)),
            pltpu.SemaphoreType.DMA((2,)),
        ] + GATHER_SEMS,
        compiler_params=pltpu.CompilerParams(
            collective_id=0, has_side_effects=True, vmem_limit_bytes=62 * 1024 * 1024),
        cost_estimate=pl.CostEstimate(flops=100000000, bytes_accessed=seq * width * 4, transcendentals=seq * HEAD_DIM * 2),
        name='first_gather',
    )(x_local, gain, wo_rows, freq)


AHEAD = 3
SPLIT = 2


def block_kernel(n, width, h_hbm, wq_hbm, wk_hbm, wv_hbm, qg_ref, kg_ref, cos_hbm, sin_hbm, next_in,
                 o_hbm, next_buf, k_out, v_out,
                 h_v, wqk_v, wv_v, cos_v, sin_v, q_s, k_s, vt_s, k_st, v_st, stats, o_s, s_buf, p_buf, acc_buf, stage,
                 h_sem, w_sem, tab_sem, kv_sem, st_send, st_recv, o_send, o_recv, o_local, *gather_sems):
    me = lax.axis_index('tp')
    tile = h_v.shape[1]
    cols = wv_v.shape[1]
    heads = cols // HEAD_DIM
    groups = tile // HEAD_DIM
    half = n // 2
    gather = RingGather(next_buf, None, stage, me, *gather_sems)
    scale = HEAD_DIM ** -0.5 * math.log2(math.e)

    def peer(d):
        return {'tp': lax.rem(me + d, n)}

    def stats_copy(chunk, d):
        part = stats.at[me, pl.ds(chunk * half, half)]
        return pltpu.make_async_remote_copy(
            src_ref=part, dst_ref=part, send_sem=st_send.at[d, chunk], recv_sem=st_recv.at[me, chunk],
            device_id=peer(d), device_id_type=MESH)

    def send_stats(chunk):
        for d in range(1, n):
            stats_copy(chunk, d).start()

    def wait_stats(chunk):
        for d in range(1, n):
            src = lax.rem(me + d, n)
            part = stats.at[src, pl.ds(chunk * half, half)]
            pltpu.make_async_remote_copy(
                src_ref=part, dst_ref=part, send_sem=st_send.at[d, chunk], recv_sem=st_recv.at[src, chunk],
                device_id=peer(d), device_id_type=MESH).wait_recv()

    def lay(x):
        return x if len(k_out.shape) == 2 else x.reshape(x.shape[0], heads, HEAD_DIM)

    def hcols(hd):
        return slice(hd * HEAD_DIM, (hd + 1) * HEAD_DIM)

    def rows_of(i):
        return pl.ds(pl.multiple_of(i * tile, tile), tile)

    def h_load(i):
        return pltpu.make_async_copy(h_hbm.at[rows_of(i)], h_v.at[i], h_sem.at[i])

    def kv_store(which, i):
        src, dst = ((k_st, k_out), (v_st, v_out))[which]
        return pltpu.make_async_copy(src.at[i], dst.at[rows_of(i)], kv_sem.at[which, i])

    w_loads = [
        pltpu.make_async_copy(wq_hbm, wqk_v.at[:, pl.ds(0, cols)], w_sem.at[0]),
        pltpu.make_async_copy(wk_hbm, wqk_v.at[:, pl.ds(cols, cols)], w_sem.at[1]),
        pltpu.make_async_copy(wv_hbm, wv_v, w_sem.at[2])]
    tab_loads = [pltpu.make_async_copy(cos_hbm, cos_v, tab_sem.at[0]), pltpu.make_async_copy(sin_hbm, sin_v, tab_sem.at[1])]

    greet(n, me)
    for load in w_loads[:2] + [h_load(i) for i in range(AHEAD)] + w_loads[2:]:
        load.start()
    pl.semaphore_wait(pltpu.get_barrier_semaphore(), n - 1)
    gather.send((0,))
    for load in w_loads[:2]:
        load.wait()

    def qk_block(i, carry):
        @pl.when(i + AHEAD < n)
        def _():
            h_load(i + AHEAD).start()

        h_load(i).wait()
        qk = jnp.dot(h_v[i], wqk_v[...], preferred_element_type=jnp.float32).astype(jnp.bfloat16)
        q, k = qk[:, :cols], qk[:, cols:]
        q_s[i] = q
        k_s[i] = k
        qf, kf = q.astype(jnp.float32), k.astype(jnp.float32)
        q_sq = jnp.sum(qf * qf, axis=1, keepdims=True)
        k_sq = jnp.sum(kf * kf, axis=1, keepdims=True)
        lane = lax.broadcasted_iota(jnp.int32, (HEAD_DIM, HEAD_DIM), 1)
        rows = []
        for g in range(groups):
            part = slice(g * HEAD_DIM, (g + 1) * HEAD_DIM)
            both = jnp.where(lane == 0, q_sq[part], k_sq[part])
            rows.append(both.T[:2])
        stats[me, i] = jnp.concatenate(rows, axis=0)
        return carry

    lax.fori_loop(0, half, qk_block, 0)
    for load in tab_loads:
        load.start()
    send_stats(0)
    gather.send((1,))
    lax.fori_loop(half, n, qk_block, 0)
    send_stats(1)
    gather.send((2, 3))
    w_loads[2].wait()

    def v_block(i, carry):
        v = jnp.dot(h_v[i], wv_v[...], preferred_element_type=jnp.float32).astype(jnp.bfloat16)
        v_st[i] = lay(v)
        kv_store(1, i).start()
        vt_s[i] = v.T
        return carry

    lax.fori_loop(0, n, v_block, 0)
    for load in tab_loads:
        load.wait()

    def norm_block(j, carry):
        total = stats[0, j]
        for src in range(1, n):
            total = total + stats[src, j]
        inv = lax.rsqrt(total / width + EPS)
        inv_cols = jnp.concatenate([inv] * (HEAD_DIM // inv.shape[0]), axis=0).T
        for g in range(groups):
            part = slice(g * HEAD_DIM, (g + 1) * HEAD_DIM)
            tab = pl.ds(pl.multiple_of(j * tile + g * HEAD_DIM, HEAD_DIM), HEAD_DIM)
            cos, sin = cos_v[tab, :], sin_v[tab, :]
            for x_s, g_ref, col in ((q_s, qg_ref, 2 * g), (k_s, kg_ref, 2 * g + 1)):
                x = x_s[j, part, :].astype(jnp.float32) * inv_cols[:, col:col + 1] * g_ref[...]
                outs = []
                for hd in range(heads):
                    xh = x[:, hcols(hd)]
                    outs.append((xh * cos + pltpu.roll(xh, HEAD_DIM // 2, 1) * sin).astype(jnp.bfloat16))
                rot = jnp.concatenate(outs, axis=1)
                x_s[j, part, :] = rot
                if x_s is k_s:
                    k_st[j, part] = lay(rot)
        kv_store(0, j).start()
        return carry

    wait_stats(0)
    lax.fori_loop(0, half, norm_block, 0)
    wait_stats(1)
    lax.fori_loop(half, n, norm_block, 0)

    def o_copy(d):
        return pltpu.make_async_remote_copy(
            src_ref=o_s.at[d], dst_ref=o_hbm.at[:, pl.ds(pl.multiple_of(me * cols, cols), cols)],
            send_sem=o_send.at[d], recv_sem=o_recv.at[me], device_id=peer(d), device_id_type=MESH)

    def o_own():
        return pltpu.make_async_copy(o_s.at[0], o_hbm.at[:, pl.ds(pl.multiple_of(me * cols, cols), cols)], o_local)

    nt = (((1,), (1,)), ((), ()))
    strip = 64

    span = tile // SPLIT
    chains = [(hd, part) for hd in range(heads) for part in range(SPLIT)]

    def softmax_step(j, chain, m, l, keys):
        hd, part = chain
        qs = slice(part * span, (part + 1) * span)
        top = None
        for c in range(keys // strip):
            best = jnp.max(s_buf[hd, c * strip:(c + 1) * strip, qs].reshape(strip // 8, 8, span), axis=0)
            top = best if top is None else jnp.maximum(top, best)
        m_new = jnp.max(top, axis=0, keepdims=True)
        if m is not None:
            m_new = jnp.maximum(m, m_new)
        m_scaled = m_new * scale
        total = None
        for c in range(keys // strip):
            p = jnp.exp2(s_buf[hd, c * strip:(c + 1) * strip, qs] * scale - m_scaled)
            add = jnp.sum(p.reshape(strip // 8, 8, span), axis=0)
            total = add if total is None else total + add
            p_buf[hd, c * strip:(c + 1) * strip, qs] = p.astype(jnp.bfloat16)
        l_new = jnp.sum(total, axis=0, keepdims=True)
        pv = jnp.dot(vt_s[j, hcols(hd), :keys], p_buf[hd, :keys, qs], preferred_element_type=jnp.float32)
        if m is None:
            acc_buf[hd, :, qs] = pv
        else:
            alpha = jnp.exp2((m - m_new) * scale)
            l_new = l * alpha + l_new
            acc_buf[hd, :, qs] = acc_buf[hd, :, qs] * alpha + pv
        return m_new, l_new

    def attend(step, carry):
        @pl.when(step == half)
        def _():
            gather.take((3, 7))

        d = lax.rem(step + 1, n)
        blk = lax.rem(me + d, n)

        def scores(j, chain, keys=tile):
            hd, part = chain
            return lax.dot_general(k_s[j, :keys, hcols(hd)], q_s[blk, part * span:(part + 1) * span, hcols(hd)], nt,
                                   preferred_element_type=jnp.float32)

        for hd, part in chains:
            keys = (part + 1) * span
            keep = (lax.broadcasted_iota(jnp.int32, (keys, span), 0)
                    <= lax.broadcasted_iota(jnp.int32, (keys, span), 1) + part * span)
            s_buf[hd, :keys, part * span:keys] = jnp.where(keep, scores(blk, (hd, part), keys), -jnp.inf)
        state = tuple(softmax_step(blk, chain, None, None, (chain[1] + 1) * span) for chain in chains)

        def body(j, state):
            for hd, part in chains:
                s_buf[hd, :, part * span:(part + 1) * span] = scores(j, (hd, part))
            return tuple(softmax_step(j, chain, *state[c], tile) for c, chain in enumerate(chains))

        state = lax.fori_loop(0, blk, body, state)
        for c, (hd, part) in enumerate(chains):
            qs = slice(part * span, (part + 1) * span)
            o_s[d, qs, hcols(hd)] = (acc_buf[hd, :, qs] / state[c][1]).T.astype(jnp.bfloat16)

        @pl.when(d != 0)
        def _():
            o_copy(d).start()

        @pl.when(d == 0)
        def _():
            o_own().start()
        return carry

    gather.relay()
    lax.fori_loop(0, n, attend, 0)
    gather.finish()
    o_own().wait()
    for d in range(1, n):
        src = lax.rem(me + d, n)
        o_copy(d).wait_send()
        pltpu.make_async_remote_copy(
            src_ref=o_s.at[d], dst_ref=o_hbm.at[:, pl.ds(pl.multiple_of(src * cols, cols), cols)],
            send_sem=o_send.at[d], recv_sem=o_recv.at[src], device_id=peer(d), device_id_type=MESH).wait_recv()
        for chunk in range(2):
            stats_copy(chunk, d).wait_send()
    for i in range(n):
        for which in range(2):
            kv_store(which, i).wait()


def block_call(n, h_full, wq, wk, wv, qg, kg, cos, sin, next_buf, cached):
    seq, width = h_full.shape
    cols = wq.shape[1]
    tile = seq // n
    heads = cols // HEAD_DIM
    next_rows = next_buf.shape[0] // n
    cache_tail = (heads, HEAD_DIM) if cached else (cols,)
    hbm = pl.BlockSpec(memory_space=pl.ANY)
    vmem = pl.BlockSpec(memory_space=pltpu.VMEM)
    flops = 2 * seq * width * cols * 3 + 2 * seq * seq * cols * 2
    cache = jax.ShapeDtypeStruct((seq,) + cache_tail, jnp.bfloat16)
    return pl.pallas_call(
        functools.partial(block_kernel, n, width),
        in_specs=[hbm, hbm, hbm, hbm, vmem, vmem, hbm, hbm, hbm],
        out_specs=[hbm, hbm, hbm, hbm],
        out_shape=[
            jax.ShapeDtypeStruct((tile, n * cols), jnp.bfloat16),
            jax.ShapeDtypeStruct(next_buf.shape, next_buf.dtype),
            cache, cache,
        ],
        input_output_aliases={8: 1},
        scratch_shapes=[
            pltpu.VMEM((n, tile, width), jnp.bfloat16),
            pltpu.VMEM((width, 2 * cols), jnp.bfloat16),
            pltpu.VMEM((width, cols), jnp.bfloat16),
            pltpu.VMEM((seq, HEAD_DIM), jnp.float32),
            pltpu.VMEM((seq, HEAD_DIM), jnp.float32),
            pltpu.VMEM((n, tile, cols), jnp.bfloat16),
            pltpu.VMEM((n, tile, cols), jnp.bfloat16),
            pltpu.VMEM((n, cols, tile), jnp.bfloat16),
            pltpu.VMEM((n, tile) + cache_tail, jnp.bfloat16),
            pltpu.VMEM((n, tile) + cache_tail, jnp.bfloat16),
            pltpu.VMEM((n, n, 2 * tile // HEAD_DIM, HEAD_DIM), jnp.float32),
            pltpu.VMEM((n, tile, cols), jnp.bfloat16),
            pltpu.VMEM((heads, tile, tile), jnp.float32),
            pltpu.VMEM((heads, tile, tile), jnp.bfloat16),
            pltpu.VMEM((heads, HEAD_DIM, tile), jnp.float32),
            pltpu.VMEM((3, next_rows, width), jnp.bfloat16),
            pltpu.SemaphoreType.DMA((n,)),
            pltpu.SemaphoreType.DMA((3,)),
            pltpu.SemaphoreType.DMA((2,)),
            pltpu.SemaphoreType.DMA((2, n)),
            pltpu.SemaphoreType.DMA((n, 2)),
            pltpu.SemaphoreType.DMA((n, 2)),
            pltpu.SemaphoreType.DMA((n,)),
            pltpu.SemaphoreType.DMA((n,)),
            pltpu.SemaphoreType.DMA,
        ] + GATHER_SEMS,
        compiler_params=pltpu.CompilerParams(
            collective_id=1 if cached else 2, has_side_effects=True, vmem_limit_bytes=62 * 1024 * 1024),
        cost_estimate=pl.CostEstimate(flops=flops, bytes_accessed=seq * width * 2 + 6 * seq * cols * 2, transcendentals=seq * seq * heads // 2),
        name='attn_block' if cached else 'attn_last',
    )(h_full, wq, wk, wv, qg, kg, cos, sin, next_buf)


N_CHUNK = 8


def last_kernel(n_batch, *refs):
    x_ref, wo_hbm = refs[:2]
    o_hbm = refs[2:2 + n_batch]
    rest = refs[2 + n_batch:]
    caches = rest[:2 * (n_batch - 1)]
    k_last, v_last = rest[2 * (n_batch - 1):2 * n_batch]
    out_ref, k_cache, v_cache = rest[2 * n_batch:2 * n_batch + 3]
    w_v, o_v, c_v, l_v, w_sem, o_sem, ci_sem, co_sem, lo_sem = rest[2 * n_batch + 3:]
    step = pl.program_id(0)
    b, j = step // N_CHUNK, lax.rem(step, N_CHUNK)
    chunk = w_v.shape[2]
    rows = c_v.shape[1]
    per = caches[0].shape[0] // rows
    slots = c_v.shape[0]

    def w_copy(c):
        return pltpu.make_async_copy(wo_hbm.at[:, pl.ds(c * chunk, chunk)], w_v.at[c], w_sem.at[c])

    def o_copy(i):
        return pltpu.make_async_copy(o_hbm[i], o_v.at[i], o_sem.at[i])

    @pl.when(step == 0)
    def _():
        w_copy(0).start()
        o_copy(0).start()
        for c in range(1, N_CHUNK):
            w_copy(c).start()
        for i in range(1, n_batch):
            o_copy(i).start()

    for i in range(n_batch):
        @pl.when(step == i * N_CHUNK)
        def _(i=i):
            o_copy(i).wait()
    for c in range(N_CHUNK):
        @pl.when(step == c)
        def _(c=c):
            w_copy(c).wait()

    items = [(i, part) for i in range(len(caches)) for part in range(per)]

    def item_in(t):
        i, part = items[t]
        return pltpu.make_async_copy(caches[i].at[pl.ds(part * rows, rows)], c_v.at[t % slots], ci_sem.at[t % slots])

    def item_out(t):
        i, part = items[t]
        cache = k_cache if i % 2 == 0 else v_cache
        return pltpu.make_async_copy(c_v.at[t % slots], cache.at[i // 2, pl.ds(part * rows, rows)], co_sem.at[t % slots])

    for t in range(len(items) + slots):
        @pl.when(step == t)
        def _(t=t):
            if t >= slots:
                item_out(t - slots).wait()
            if t < len(items):
                item_in(t).start()
            if 1 <= t <= len(items):
                item_in(t - 1).wait()
                item_out(t - 1).start()

    last_rows = l_v.shape[2]

    def last_out(which, t):
        cache = (k_cache, v_cache)[which]
        return pltpu.make_async_copy(l_v.at[which, lax.rem(t, 2)],
                                     cache.at[n_batch - 1, pl.ds(pl.multiple_of(t * last_rows, last_rows), last_rows)],
                                     lo_sem.at[which, lax.rem(t, 2)])

    @pl.when(step >= 2)
    def _():
        for which in range(2):
            last_out(which, step - 2).wait()
    for which, src in enumerate((k_last, v_last)):
        l_v[which, lax.rem(step, 2)] = src[...].reshape(l_v.shape[2:])
        last_out(which, step).start()

    y = jnp.dot(o_v[b], w_v[j], preferred_element_type=jnp.float32).astype(jnp.bfloat16)
    out_ref[0] = (x_ref[0].astype(jnp.float32) + y.astype(jnp.float32)).astype(jnp.bfloat16)

    @pl.when(step == n_batch * N_CHUNK - 1)
    def _():
        for which in range(2):
            for back in (1, 0):
                last_out(which, step - back).wait()


def last_call(x_local, w_o, os, ks, vs):
    n_batch, rows, width = x_local.shape
    seq, heads, _ = ks[0].shape
    steps = n_batch * N_CHUNK
    hbm = pl.BlockSpec(memory_space=pl.ANY)
    block = pl.BlockSpec((1, rows, width // N_CHUNK), lambda i: (i // N_CHUNK, 0, lax.rem(i, N_CHUNK)))
    last = pl.BlockSpec((seq // steps, heads * HEAD_DIM), lambda i: (i, 0))
    caches = [c for pair in zip(ks[:-1], vs[:-1]) for c in pair]
    cache = jax.ShapeDtypeStruct((n_batch, seq, heads, HEAD_DIM), jnp.bfloat16)
    return pl.pallas_call(
        functools.partial(last_kernel, n_batch),
        grid=(steps,),
        in_specs=[block, hbm] + [hbm] * (n_batch + len(caches)) + [last, last],
        out_specs=[block, hbm, hbm],
        out_shape=[jax.ShapeDtypeStruct(x_local.shape, jnp.bfloat16), cache, cache],
        scratch_shapes=[
            pltpu.VMEM((N_CHUNK, w_o.shape[0], width // N_CHUNK), jnp.bfloat16),
            pltpu.VMEM((n_batch, rows, w_o.shape[0]), jnp.bfloat16),
            pltpu.VMEM((4, 2048, heads, HEAD_DIM), jnp.bfloat16),
            pltpu.VMEM((2, 2, seq // steps, heads, HEAD_DIM), jnp.bfloat16),
            pltpu.SemaphoreType.DMA((N_CHUNK,)),
            pltpu.SemaphoreType.DMA((n_batch,)),
            pltpu.SemaphoreType.DMA((4,)),
            pltpu.SemaphoreType.DMA((4,)),
            pltpu.SemaphoreType.DMA((2, 2)),
        ],
        compiler_params=pltpu.CompilerParams(
            vmem_limit_bytes=52 * 1024 * 1024, dimension_semantics=('arbitrary',)),
        cost_estimate=pl.CostEstimate(flops=2 * n_batch * rows * width * w_o.shape[0],
                                      bytes_accessed=8 * n_batch * rows * width * 2, transcendentals=0),
        name='last_proj',
    )(x_local, w_o, *os, *caches, ks[-1], vs[-1])


def solution(mesh):
    n = mesh.shape['tp']
    assert n == 8 and tuple(mesh.axis_names) == ('dp', 'tp')

    def local_block(x_local, attn_gain, wq, wk, wv, qg, kg, wo_rows):
        n_batch, rows, width = x_local.shape
        cols = wq.shape[1]
        qg2, kg2 = qg.reshape(1, cols), kg.reshape(1, cols)
        half_dim = HEAD_DIM // 2
        inv_freq = 10000.0 ** (-jnp.arange(half_dim, dtype=jnp.float32) * (2.0 / HEAD_DIM))
        freq = jnp.concatenate([inv_freq, inv_freq]).reshape(1, HEAD_DIM)
        *hs, w_o, cos, sin = first_call(n, x_local, attn_gain.reshape(1, width), wo_rows, freq)
        os, ks, vs = [], [], []
        for b in range(n_batch):
            more = b + 1 < n_batch
            o, gathered, k, v = block_call(n, hs[b], wq, wk, wv, qg2, kg2, cos, sin, hs[b + 1] if more else w_o, more)
            if more:
                hs[b + 1] = gathered
            else:
                w_o = gathered
            os.append(o)
            ks.append(k)
            vs.append(v)
        return tuple(last_call(x_local, w_o, os, ks, vs))

    seq_spec = P('dp', 'tp', None)
    head_spec = P('dp', None, 'tp', None)
    col_spec = P(None, 'tp')
    return jax.shard_map(local_block, mesh=mesh, in_specs=(seq_spec, P(None), col_spec, col_spec, col_spec, P('tp'), P('tp'), P('tp', None)), out_specs=(seq_spec, head_spec, head_spec), check_vma=False)
```
